32 devices in a mesh: pb: 8 (over z, x), ka: 4 (over y, core).
Axes of the slice: x: 2, y: 2, z: 4, core: 2. Of those that a mesh axis runs over, the one named last changes fastest.
Arguments:
- query_saved: bfloat16 [1024, 1024], P(('pb', 'ka')), may hold values from -6 to 6
- key_saved: bfloat16 [2048, 1024], P(('ka', 'pb')), may hold values from -6 to 6
- value_saved: bfloat16 [2048, 1024], P(('ka', 'pb')), may hold values from -6 to 6
- out_grad: bfloat16 [1024, 1024], P(('pb', 'ka')), may hold values from -768 to 768
- log_norm: bfloat16 [16, 1024], P(None, ('pb', 'ka')), as said below
- row_delta: bfloat16 [16, 1024], P(None, ('pb', 'ka')), may hold values from -1536 to 1536
- weight_query: bfloat16 [1024, 1024], replicated, may hold values from -0.1875 to 0.1875
- weight_key: bfloat16 [1024, 1024], replicated, may hold values from -0.1875 to 0.1875
- weight_value: bfloat16 [1024, 1024], replicated, may hold values from -0.1875 to 0.1875
Outputs:
- dx_query: bfloat16 [1024, 1024], P(('pb', 'ka'))
- dx_keyvalue: bfloat16 [2048, 1024], P(('ka', 'pb'))
The draws below stay inside these ranges and needn't reach their ends.
Inputs may be any that keep to these rules, and one draw needn't show every extreme that they name: `log_norm`: each entry lies within 2 of 0.5 plus the natural logarithm of 2048.
All inputs are finite; a program needn't handle non-finite values.
Results may differ from the reference program's by a relative error of at most 0.008.
Values may be sent and summed in bfloat16 or wider, within the bound.
No kernel may reach another device: no remote copies, remote signals or barrier semaphores. Data moves between devices by JAX's collectives and lax.ppermute only.
A program may use at most 128 MiB of HBM per device.

```python
import jax
import jax.numpy as jnp
from jax import lax

D = 1024
HEAD_DIM = 64
QTOK_DEV = 32
HEADS = 16
TOKENS = 2048
QUERIES = 1024
N_KA = 4


def draw_log_norm(key, part):
    jitter = jax.random.uniform(key, (HEADS, QUERIES), jnp.float32, -1.0, 1.0)
    return (jnp.log(jnp.float32(TOKENS)) + 0.5 + jitter).astype(jnp.bfloat16)


def level_of(stream_key, shape, split, smallest, top_value):
    loudness = 1.0
    for dim, parts in split:
        draws = jax.random.uniform(jax.random.fold_in(jax.random.fold_in(stream_key, 6), dim), (parts,), jnp.float32, smallest / len(split), top_value / len(split))
        loudness = loudness * jnp.repeat(jnp.exp(draws), shape[dim] // parts).reshape((-1,) + (1,) * (len(shape) - 1 - dim))
    return loudness


def scatter_about(own_key, extent, scale, most, shards=(), held_as=jnp.bfloat16):
    entries = scale * jax.random.normal(own_key, extent, jnp.float32)
    if shards:
        entries = entries * level_of(own_key, extent, shards, -0.22, 0.18)
    return jnp.clip(entries, -most, most).astype(held_as)


def setup_inputs(seed: int = 0) -> dict:
    splits = jax.random.split(jax.random.key(seed), 10)
    query_saved = scatter_about(splits[0], (QUERIES, D), 1.0, 6.0, ((0, 32),))
    key_saved = scatter_about(splits[1], (TOKENS, D), 1.0, 6.0, ((0, 32),))
    value_saved = scatter_about(splits[2], (TOKENS, D), 1.0, 6.0, ((0, 32),))
    out_grad = scatter_about(splits[3], (QUERIES, D), 128.0, 768.0, ((0, 32),))
    log_norm = draw_log_norm(jax.random.fold_in(splits[9], 71), 0)
    row_delta = scatter_about(splits[5], (HEADS, QUERIES), 256.0, 1536.0, ((1, 32),))
    weight_query = scatter_about(splits[6], (D, D), D ** -0.5, 0.1875)
    weight_key = scatter_about(splits[7], (D, D), D ** -0.5, 0.1875)
    weight_value = scatter_about(splits[8], (D, D), D ** -0.5, 0.1875)
    return {"query_saved": query_saved, "key_saved": key_saved, "value_saved": value_saved, "out_grad": out_grad, "log_norm": log_norm, "row_delta": row_delta, "weight_query": weight_query, "weight_key": weight_key, "weight_value": weight_value}


def reference(query_saved, key_saved, value_saved, out_grad, log_norm, row_delta, weight_query, weight_key, weight_value):
    query_total = query_saved.shape[0]
    key_total = key_saved.shape[0]
    block_rows = QTOK_DEV * N_KA
    blocks = query_total // block_rows
    head_count = D // HEAD_DIM
    score_scale = 1.0 / (HEAD_DIM ** 0.5)

    def per_head(head_index):
        column = head_index * HEAD_DIM
        queries = lax.dynamic_slice_in_dim(query_saved, column, HEAD_DIM, 1)
        keys_head = lax.dynamic_slice_in_dim(key_saved, column, HEAD_DIM, 1)
        values_head = lax.dynamic_slice_in_dim(value_saved, column, HEAD_DIM, 1)
        grads_head = lax.dynamic_slice_in_dim(out_grad, column, HEAD_DIM, 1)
        norm_row = lax.dynamic_index_in_dim(log_norm, head_index, 0, keepdims=False).astype(jnp.float32)
        delta_row = lax.dynamic_index_in_dim(row_delta, head_index, 0, keepdims=False).astype(jnp.float32)

        def query_step(totals, block_index):
            grad_key, grad_value = totals
            first_row = (block_index * block_rows).astype(jnp.int32)
            query_block = lax.dynamic_slice_in_dim(queries, first_row, block_rows, 0)
            grad_block = lax.dynamic_slice_in_dim(grads_head, first_row, block_rows, 0)
            norm_block = lax.dynamic_slice_in_dim(norm_row, first_row, block_rows, 0)
            delta_block = lax.dynamic_slice_in_dim(delta_row, first_row, block_rows, 0)
            scores = jnp.dot(query_block, keys_head.T, preferred_element_type=jnp.float32) * score_scale
            probs = jnp.exp(scores - norm_block[:, None])
            probs_b = probs.astype(jnp.bfloat16)
            grad_probs = jnp.dot(grad_block, values_head.T, preferred_element_type=jnp.float32)
            grad_scores = probs * (grad_probs - delta_block[:, None])
            grad_scores_b = grad_scores.astype(jnp.bfloat16)
            grad_value = grad_value + jnp.dot(probs_b.T, grad_block, preferred_element_type=jnp.float32)
            grad_key = grad_key + jnp.dot(grad_scores_b.T, query_block, preferred_element_type=jnp.float32) * score_scale
            grad_query = jnp.dot(grad_scores_b, keys_head, preferred_element_type=jnp.float32) * score_scale
            return (grad_key, grad_value), grad_query

        start_totals = (jnp.zeros((key_total, HEAD_DIM), jnp.float32), jnp.zeros((key_total, HEAD_DIM), jnp.float32))
        (grad_key, grad_value), query_parts = lax.scan(query_step, start_totals, jnp.arange(blocks, dtype=jnp.int32))
        return query_parts.reshape(query_total, HEAD_DIM), grad_key, grad_value

    grad_query, grad_key, grad_value = lax.map(per_head, jnp.arange(head_count, dtype=jnp.int32))

    def merge_heads(stacked, row_count):
        return jnp.transpose(stacked, (1, 0, 2)).reshape(row_count, D)

    grad_query = merge_heads(grad_query, query_total)
    grad_key = merge_heads(grad_key, key_total)
    grad_value = merge_heads(grad_value, key_total)
    contract = (((1,), (1,)), ((), ()))

    def project(grads, weights):
        return lax.dot_general(grads, weights.astype(jnp.float32), contract, precision=lax.Precision.HIGHEST, preferred_element_type=jnp.float32)

    dx_query = project(grad_query, weight_query).astype(jnp.bfloat16)
    dx_keyvalue = (project(grad_key, weight_key) + project(grad_value, weight_value)).astype(jnp.bfloat16)
    return (dx_query, dx_keyvalue)
```

```python
import functools
import math

import jax
import jax.numpy as jnp
from jax import lax
from jax.experimental import pallas as pl
from jax.experimental.pallas import tpu as pltpu
from jax.sharding import PartitionSpec as P

HEAD_DIM = 64
LANES = 2 * HEAD_DIM
SCALE = 1.0 / HEAD_DIM**0.5
LOG2E = math.log2(math.e)
EXTRA = 8
TILE = 256
AXES = ("pb", "ka")
F32 = jnp.float32
BF16 = jnp.bfloat16
ROWS_BY_ROWS = (((1,), (1,)), ((), ()))


def low_lanes(rows):
    return lax.broadcasted_iota(jnp.int32, (rows, LANES), 1) < HEAD_DIM


def regroup(first, second):
    low = low_lanes(first.shape[0])
    mixed = pltpu.roll(jnp.where(low, second, first), HEAD_DIM, 1)
    return jnp.where(low, first, mixed), jnp.where(low, mixed, second)


def pack_kernel(n_ka, reps, sec, q_ref, k_ref, v_ref, g_ref, norm_ref, delta_ref, out_ref):
    heads, rows = norm_ref.shape
    kept = k_ref.shape[1]
    half = rows // 2
    me = lax.axis_index("pb") * n_ka + lax.axis_index("ka")
    slot = lax.rem(me, LANES // half)
    token = lax.broadcasted_iota(jnp.int32, (rows, 2 * LANES), 0)
    lane = lax.broadcasted_iota(jnp.int32, (rows, 2 * LANES), 1)
    target = slot * half + token + jnp.where(token < half, 0, LANES - half)
    place = jnp.where(lane == target, 1.0, 0.0).astype(BF16)
    both = jnp.concatenate([norm_ref[...], delta_ref[...]], axis=0)
    moved = jnp.dot(both, place, preferred_element_type=F32)
    stacked = jnp.concatenate(
        [
            moved[:heads, :LANES],
            moved[:heads, LANES:],
            moved[heads:, :LANES],
            moved[heads:, LANES:],
        ],
        axis=0,
    ).astype(BF16)
    row = lax.broadcasted_iota(jnp.int32, (heads * EXTRA, 4 * heads), 0)
    col = lax.broadcasted_iota(jnp.int32, (heads * EXTRA, 4 * heads), 1)
    kind = lax.rem(row, EXTRA)
    wanted = kind * heads + lax.div(row, EXTRA)
    pick = jnp.where((col == wanted) & (kind < 4), 1.0, 0.0).astype(BF16)
    extra = jnp.dot(pick, stacked, preferred_element_type=F32)

    for pair in range(heads // 2):
        cols = slice(pair * LANES, (pair + 1) * LANES)
        queries = regroup(q_ref[:, cols].astype(F32), g_ref[:, cols].astype(F32))
        keys = [
            regroup(k_ref[rep, :, cols].astype(F32), v_ref[rep, :, cols].astype(F32))
            for rep in range(reps)
        ]
        for side in range(2):
            head = 2 * pair + side
            query_rows = queries[side].astype(BF16)
            extra_rows = extra[head * EXTRA : (head + 1) * EXTRA].astype(BF16)
            for rep in range(reps):
                chunk = head * reps + rep
                out_ref[chunk, 0:rows, :] = query_rows
                if kept < sec:
                    out_ref[chunk, rows : rows + sec, :] = jnp.zeros((sec, LANES), BF16)
                out_ref[chunk, rows : rows + kept, :] = keys[rep][side].astype(BF16)
                out_ref[chunk, rows + sec : rows + sec + EXTRA, :] = extra_rows


def attend_kernel(rows, sec, in_ref, out_ref, kv_ref, kt_ref, acc_ref):
    count = in_ref.shape[0]
    half = rows // 2
    sources = TILE // half
    slots = LANES // half
    key_tiles = count * sec // TILE
    per_tile = TILE // sec
    low = low_lanes(TILE)

    for tile in range(key_tiles):
        part = in_ref[tile * per_tile : (tile + 1) * per_tile, rows : rows + sec, :]
        part = part.astype(F32).reshape(TILE, LANES)
        kv_ref[tile * TILE : (tile + 1) * TILE, :] = part.astype(BF16)
        kt_ref[:, tile * TILE : (tile + 1) * TILE] = part.T[:HEAD_DIM].astype(BF16)
    acc_ref[...] = jnp.zeros_like(acc_ref)

    def group(index):
        base = index * sources
        saved = jnp.concatenate(
            [
                in_ref[pl.ds(base + part * slots, slots), rows + sec : rows + sec + EXTRA, :]
                .astype(F32)
                .sum(0)
                for part in range(TILE // LANES)
            ],
            axis=1,
        )
        sides = []
        for side in range(2):
            block = in_ref[pl.ds(base, sources), side * half : (side + 1) * half, :]
            block = block.reshape(TILE, LANES).astype(F32)
            queries = jnp.where(low, block * SCALE, 0.0).astype(BF16)
            grads = jnp.where(low, 0.0, block).astype(BF16)
            norm = saved[side : side + 1] * LOG2E
            delta = saved[2 + side : 3 + side]
            grad_query = jnp.zeros((HEAD_DIM, TILE), F32)
            for tile in range(key_tiles):
                span = slice(tile * TILE, (tile + 1) * TILE)
                kv = kv_ref[span, :]
                scores = lax.dot_general(kv, queries, ROWS_BY_ROWS, preferred_element_type=F32)
                grad_probs = lax.dot_general(kv, grads, ROWS_BY_ROWS, preferred_element_type=F32)
                probs = jnp.exp2(scores * LOG2E - norm)
                grad_scores = (probs * (grad_probs - delta)).astype(BF16)
                probs = probs.astype(BF16)
                acc_ref[span, :] += jnp.dot(
                    grad_scores, queries, preferred_element_type=F32
                ) + jnp.dot(probs, grads, preferred_element_type=F32)
                grad_query += jnp.dot(kt_ref[:, span], grad_scores, preferred_element_type=F32)
            sides.append(grad_query)
        packed = (jnp.concatenate(sides, axis=0).T * SCALE).astype(BF16)
        out_ref[pl.ds(base, sources), sec : sec + half, :] = packed.reshape(sources, half, LANES)

    groups = count // sources
    if groups <= 2:
        for index in range(groups):
            group(index)
    else:
        lax.fori_loop(0, groups, lambda index, _: (group(index), 0)[1], 0)

    for tile in range(key_tiles):
        part = acc_ref[tile * TILE : (tile + 1) * TILE, :].reshape(per_tile, sec, LANES)
        out_ref[tile * per_tile : (tile + 1) * per_tile, 0:sec, :] = part.astype(BF16)


def project_kernel(
    reps, sec, in_ref, wq_ref, wk_ref, wv_ref, dxq_ref, dxkv_ref, gq_ref, gk_ref, gv_ref
):
    heads = in_ref.shape[0] // reps
    half = in_ref.shape[1] - sec
    for pair in range(heads // 2):
        cols = slice(pair * LANES, (pair + 1) * LANES)
        for rep in range(reps):
            even, odd = (
                in_ref[(2 * pair + side) * reps + rep, 0:sec, :].astype(F32) for side in range(2)
            )
            grad_key, grad_value = regroup(even, odd)
            span = slice(rep * sec, (rep + 1) * sec)
            gk_ref[span, cols] = grad_key.astype(BF16)
            gv_ref[span, cols] = grad_value.astype(BF16)
        even, odd = (
            in_ref[(2 * pair + side) * reps : (2 * pair + side + 1) * reps, sec : sec + half, :]
            .astype(F32)
            .sum(0)
            for side in range(2)
        )
        early, late = regroup(even, odd)
        gq_ref[0:half, cols] = early.astype(BF16)
        gq_ref[half : 2 * half, cols] = late.astype(BF16)

    def times(grads_ref, weight_ref):
        return lax.dot_general(
            grads_ref[...], weight_ref[...], ROWS_BY_ROWS, preferred_element_type=F32
        )

    dxq_ref[...] = times(gq_ref, wq_ref).astype(BF16)
    dxkv_ref[...] = (times(gk_ref, wk_ref) + times(gv_ref, wv_ref)).astype(BF16)


def vmem(count):
    return [pl.BlockSpec(memory_space=pltpu.VMEM)] * count


def local(
    n_ka,
    count,
    query_saved,
    key_saved,
    value_saved,
    out_grad,
    log_norm,
    row_delta,
    weight_query,
    weight_key,
    weight_value,
):
    rows, width = query_saved.shape
    key_rows = key_saved.shape[0]
    heads = width // HEAD_DIM
    reps = count // heads
    kept = key_rows // reps
    sec = -(-kept // 8) * 8
    half = rows // 2
    keys = count * sec

    sent = pl.pallas_call(
        functools.partial(pack_kernel, n_ka, reps, sec),
        out_shape=jax.ShapeDtypeStruct((count, rows + sec + EXTRA, LANES), BF16),
        in_specs=vmem(6),
        out_specs=pl.BlockSpec(memory_space=pltpu.VMEM),
    )(
        query_saved,
        key_saved.reshape(reps, kept, width),
        value_saved.reshape(reps, kept, width),
        out_grad,
        log_norm,
        row_delta,
    )
    held = lax.all_to_all(sent, AXES, 0, 0)
    grads = pl.pallas_call(
        functools.partial(attend_kernel, rows, sec),
        out_shape=jax.ShapeDtypeStruct((count, sec + half, LANES), BF16),
        in_specs=vmem(1),
        out_specs=pl.BlockSpec(memory_space=pltpu.VMEM),
        scratch_shapes=[
            pltpu.VMEM((keys, LANES), BF16),
            pltpu.VMEM((HEAD_DIM, keys), BF16),
            pltpu.VMEM((keys, LANES), F32),
        ],
    )(held)
    returned = lax.all_to_all(grads, AXES, 0, 0)
    dx_query, dx_keyvalue = pl.pallas_call(
        functools.partial(project_kernel, reps, sec),
        out_shape=(
            jax.ShapeDtypeStruct((rows, width), BF16),
            jax.ShapeDtypeStruct((reps * sec, width), BF16),
        ),
        in_specs=vmem(4),
        out_specs=tuple(vmem(2)),
        scratch_shapes=[
            pltpu.VMEM((rows, width), BF16),
            pltpu.VMEM((reps * sec, width), BF16),
            pltpu.VMEM((reps * sec, width), BF16),
        ],
    )(returned, weight_query, weight_key, weight_value)
    if kept != sec:
        dx_keyvalue = dx_keyvalue.reshape(reps, sec, width)[:, :kept].reshape(key_rows, width)
    return dx_query, dx_keyvalue


def solution(mesh):
    n_ka = mesh.shape["ka"]
    count = mesh.shape["pb"] * n_ka
    in_specs = (
        P(("pb", "ka"), None),
        P(("ka", "pb"), None),
        P(("ka", "pb"), None),
        P(("pb", "ka"), None),
        P(None, ("pb", "ka")),
        P(None, ("pb", "ka")),
        P(),
        P(),
        P(),
    )
    out_specs = (P(("pb", "ka"), None), P(("ka", "pb"), None))
    return jax.shard_map(
        functools.partial(local, n_ka, count),
        mesh=mesh,
        in_specs=in_specs,
        out_specs=out_specs,
        check_vma=False,
    )
```

```python
import functools
import math

import jax
import jax.numpy as jnp
from jax import lax
from jax.experimental import pallas as pl
from jax.experimental.pallas import tpu as pltpu
from jax.sharding import PartitionSpec as P

HEAD_DIM = 64
LANES = 2 * HEAD_DIM
SCALE = 1.0 / HEAD_DIM**0.5
LOG2E = math.log2(math.e)
PARAMS = pltpu.CompilerParams(vmem_limit_bytes=24 * 1024 * 1024)
EXTRA = 8
TILE = 256
AXES = ("pb", "ka")
F32 = jnp.float32
BF16 = jnp.bfloat16
ROWS_BY_ROWS = (((1,), (1,)), ((), ()))


def low_lanes(rows):
    return lax.broadcasted_iota(jnp.int32, (rows, LANES), 1) < HEAD_DIM


def regroup(first, second):
    low = low_lanes(first.shape[0])
    mixed = pltpu.roll(jnp.where(low, second, first), HEAD_DIM, 1)
    return jnp.where(low, first, mixed), jnp.where(low, mixed, second)


def pack_kernel(n_ka, reps, sec, *refs):
    sources, out_ref, (*held, sems) = refs[:6], refs[6], refs[7:]
    copies = [
        pltpu.make_async_copy(source, target, sems.at[index])
        for index, (source, target) in enumerate(zip(sources, held))
    ]
    for copy in copies:
        copy.start()
    for copy in copies:
        copy.wait()
    q_ref, g_ref, k_ref, v_ref, norm_ref, delta_ref = held
    heads, rows = norm_ref.shape
    kept = k_ref.shape[1]
    half = rows // 2
    me = lax.axis_index("pb") * n_ka + lax.axis_index("ka")
    slot = lax.rem(me, LANES // half)
    token = lax.broadcasted_iota(jnp.int32, (rows, 2 * LANES), 0)
    lane = lax.broadcasted_iota(jnp.int32, (rows, 2 * LANES), 1)
    target = slot * half + token + jnp.where(token < half, 0, LANES - half)
    place = jnp.where(lane == target, 1.0, 0.0).astype(BF16)
    both = jnp.concatenate([norm_ref[...], delta_ref[...]], axis=0)
    moved = jnp.dot(both, place, preferred_element_type=F32)
    stacked = jnp.concatenate(
        [
            moved[:heads, :LANES],
            moved[:heads, LANES:],
            moved[heads:, :LANES],
            moved[heads:, LANES:],
        ],
        axis=0,
    ).astype(BF16)
    row = lax.broadcasted_iota(jnp.int32, (heads * EXTRA, 4 * heads), 0)
    col = lax.broadcasted_iota(jnp.int32, (heads * EXTRA, 4 * heads), 1)
    kind = lax.rem(row, EXTRA)
    wanted = kind * heads + lax.div(row, EXTRA)
    pick = jnp.where((col == wanted) & (kind < 4), 1.0, 0.0).astype(BF16)
    extra = jnp.dot(pick, stacked, preferred_element_type=F32)

    for pair in range(heads // 2):
        cols = slice(pair * LANES, (pair + 1) * LANES)
        queries = regroup(q_ref[:, cols].astype(F32), g_ref[:, cols].astype(F32))
        keys = [
            regroup(k_ref[rep, :, cols].astype(F32), v_ref[rep, :, cols].astype(F32))
            for rep in range(reps)
        ]
        for side in range(2):
            head = 2 * pair + side
            query_rows = queries[side].astype(BF16)
            extra_rows = extra[head * EXTRA : (head + 1) * EXTRA].astype(BF16)
            for rep in range(reps):
                chunk = head * reps + rep
                out_ref[chunk, 0:rows, :] = query_rows
                if kept < sec:
                    out_ref[chunk, rows : rows + sec, :] = jnp.zeros((sec, LANES), BF16)
                out_ref[chunk, rows : rows + kept, :] = keys[rep][side].astype(BF16)
                out_ref[chunk, rows + sec : rows + sec + EXTRA, :] = extra_rows


def attend_kernel(rows, sec, in_ref, *refs):
    weights, out_ref, near, (kv_ref, kt_ref, acc_ref, sems) = refs[:3], refs[3], refs[4:7], refs[7:]
    copies = [
        pltpu.make_async_copy(source, target, sems.at[index])
        for index, (source, target) in enumerate(zip(weights, near))
    ]
    for copy in copies:
        copy.start()
    count = in_ref.shape[0]
    half = rows // 2
    sources = TILE // half
    slots = LANES // half
    key_tiles = count * sec // TILE
    per_tile = TILE // sec
    low = low_lanes(TILE)

    for tile in range(key_tiles):
        part = in_ref[tile * per_tile : (tile + 1) * per_tile, rows : rows + sec, :]
        part = part.astype(F32).reshape(TILE, LANES)
        kv_ref[tile * TILE : (tile + 1) * TILE, :] = part.astype(BF16)
        kt_ref[:, tile * TILE : (tile + 1) * TILE] = part.T[:HEAD_DIM].astype(BF16)
    acc_ref[...] = jnp.zeros_like(acc_ref)

    def group(index):
        base = index * sources
        saved = jnp.concatenate(
            [
                in_ref[pl.ds(base + part * slots, slots), rows + sec : rows + sec + EXTRA, :]
                .astype(F32)
                .sum(0)
                for part in range(TILE // LANES)
            ],
            axis=1,
        )
        sides = []
        for side in range(2):
            block = in_ref[pl.ds(base, sources), side * half : (side + 1) * half, :]
            block = block.reshape(TILE, LANES).astype(F32)
            queries = jnp.where(low, block * SCALE, 0.0).astype(BF16)
            grads = jnp.where(low, 0.0, block).astype(BF16)
            norm = saved[side : side + 1] * LOG2E
            delta = saved[2 + side : 3 + side]
            grad_query = jnp.zeros((HEAD_DIM, TILE), F32)
            for tile in range(key_tiles):
                span = slice(tile * TILE, (tile + 1) * TILE)
                kv = kv_ref[span, :]
                scores = lax.dot_general(kv, queries, ROWS_BY_ROWS, preferred_element_type=F32)
                grad_probs = lax.dot_general(kv, grads, ROWS_BY_ROWS, preferred_element_type=F32)
                probs = jnp.exp2(scores * LOG2E - norm)
                grad_scores = (probs * (grad_probs - delta)).astype(BF16)
                probs = probs.astype(BF16)
                acc_ref[span, :] += jnp.dot(
                    grad_scores, queries, preferred_element_type=F32
                ) + jnp.dot(probs, grads, preferred_element_type=F32)
                grad_query += jnp.dot(kt_ref[:, span], grad_scores, preferred_element_type=F32)
            sides.append(grad_query)
        packed = (jnp.concatenate(sides, axis=0).T * SCALE).astype(BF16)
        out_ref[pl.ds(base, sources), sec : sec + half, :] = packed.reshape(sources, half, LANES)

    groups = count // sources
    if groups <= 2:
        for index in range(groups):
            group(index)
    else:
        lax.fori_loop(0, groups, lambda index, _: (group(index), 0)[1], 0)

    for tile in range(key_tiles):
        part = acc_ref[tile * TILE : (tile + 1) * TILE, :].reshape(per_tile, sec, LANES)
        out_ref[tile * per_tile : (tile + 1) * per_tile, 0:sec, :] = part.astype(BF16)
    for copy in copies:
        copy.wait()


def project_kernel(
    reps, sec, in_ref, wq_ref, wk_ref, wv_ref, dxq_ref, dxkv_ref, gq_ref, gk_ref, gv_ref
):
    heads = in_ref.shape[0] // reps
    half = in_ref.shape[1] - sec
    for pair in range(heads // 2):
        cols = slice(pair * LANES, (pair + 1) * LANES)
        for rep in range(reps):
            even, odd = (
                in_ref[(2 * pair + side) * reps + rep, 0:sec, :].astype(F32) for side in range(2)
            )
            grad_key, grad_value = regroup(even, odd)
            span = slice(rep * sec, (rep + 1) * sec)
            gk_ref[span, cols] = grad_key.astype(BF16)
            gv_ref[span, cols] = grad_value.astype(BF16)
        even, odd = (
            in_ref[(2 * pair + side) * reps : (2 * pair + side + 1) * reps, sec : sec + half, :]
            .astype(F32)
            .sum(0)
            for side in range(2)
        )
        early, late = regroup(even, odd)
        gq_ref[0:half, cols] = early.astype(BF16)
        gq_ref[half : 2 * half, cols] = late.astype(BF16)

    def times(grads_ref, weight_ref):
        return lax.dot_general(
            grads_ref[...], weight_ref[...], ROWS_BY_ROWS, preferred_element_type=F32
        )

    dxq_ref[...] = times(gq_ref, wq_ref).astype(BF16)
    dxkv_ref[...] = (times(gk_ref, wk_ref) + times(gv_ref, wv_ref)).astype(BF16)


def in_vmem(count):
    return [pl.BlockSpec(memory_space=pltpu.VMEM)] * count


def in_hbm(count):
    return [pl.BlockSpec(memory_space=pltpu.HBM)] * count


def local(
    n_ka,
    count,
    query_saved,
    key_saved,
    value_saved,
    out_grad,
    log_norm,
    row_delta,
    weight_query,
    weight_key,
    weight_value,
):
    rows, width = query_saved.shape
    key_rows = key_saved.shape[0]
    heads = width // HEAD_DIM
    reps = count // heads
    kept = key_rows // reps
    sec = -(-kept // 8) * 8
    half = rows // 2
    keys = count * sec

    inputs = [
        query_saved,
        out_grad,
        key_saved.reshape(reps, kept, width),
        value_saved.reshape(reps, kept, width),
        log_norm,
        row_delta,
    ]
    sent = pl.pallas_call(
        functools.partial(pack_kernel, n_ka, reps, sec),
        out_shape=pltpu.VMEM((count, rows + sec + EXTRA, LANES), BF16),
        in_specs=in_hbm(6),
        out_specs=in_vmem(1)[0],
        scratch_shapes=[pltpu.VMEM(array.shape, BF16) for array in inputs]
        + [pltpu.SemaphoreType.DMA((6,))],
        compiler_params=PARAMS,
    )(*[pltpu.with_memory_space_constraint(array, pltpu.HBM) for array in inputs])
    held = lax.all_to_all(sent, AXES, 0, 0)
    weights = [weight_query, weight_key, weight_value]
    grads, *weights = pl.pallas_call(
        functools.partial(attend_kernel, rows, sec),
        out_shape=[pltpu.VMEM((count, sec + half, LANES), BF16)]
        + [pltpu.VMEM(weight.shape, BF16) for weight in weights],
        in_specs=in_vmem(1) + in_hbm(3),
        out_specs=in_vmem(4),
        scratch_shapes=[
            pltpu.VMEM((keys, LANES), BF16),
            pltpu.VMEM((HEAD_DIM, keys), BF16),
            pltpu.VMEM((keys, LANES), F32),
            pltpu.SemaphoreType.DMA((3,)),
        ],
        compiler_params=PARAMS,
    )(held, *[pltpu.with_memory_space_constraint(weight, pltpu.HBM) for weight in weights])
    returned = lax.all_to_all(grads, AXES, 0, 0)
    dx_query, dx_keyvalue = pl.pallas_call(
        functools.partial(project_kernel, reps, sec),
        out_shape=(
            jax.ShapeDtypeStruct((rows, width), BF16),
            jax.ShapeDtypeStruct((reps * sec, width), BF16),
        ),
        in_specs=in_vmem(4),
        out_specs=tuple(in_vmem(2)),
        scratch_shapes=[
            pltpu.VMEM((rows, width), BF16),
            pltpu.VMEM((reps * sec, width), BF16),
            pltpu.VMEM((reps * sec, width), BF16),
        ],
        compiler_params=PARAMS,
    )(returned, *weights)
    if kept != sec:
        dx_keyvalue = dx_keyvalue.reshape(reps, sec, width)[:, :kept].reshape(key_rows, width)
    return dx_query, dx_keyvalue


def solution(mesh):
    n_ka = mesh.shape["ka"]
    count = mesh.shape["pb"] * n_ka
    in_specs = (
        P(("pb", "ka"), None),
        P(("ka", "pb"), None),
        P(("ka", "pb"), None),
        P(("pb", "ka"), None),
        P(None, ("pb", "ka")),
        P(None, ("pb", "ka")),
        P(),
        P(),
        P(),
    )
    out_specs = (P(("pb", "ka"), None), P(("ka", "pb"), None))
    return jax.shard_map(
        functools.partial(local, n_ka, count),
        mesh=mesh,
        in_specs=in_specs,
        out_specs=out_specs,
        check_vma=False,
    )
```

```python
import functools
import math

import jax
import jax.numpy as jnp
from jax import lax
from jax.experimental import pallas as pl
from jax.experimental.pallas import tpu as pltpu
from jax.sharding import PartitionSpec as P

HEAD_DIM = 64
LANES = 2 * HEAD_DIM
SCALE = 1.0 / HEAD_DIM**0.5
LOG2E = math.log2(math.e)
TILE = 256
VMEM_LIMIT = 24 * 1024 * 1024
PARAMS = pltpu.CompilerParams(vmem_limit_bytes=VMEM_LIMIT)
AXES = ("pb", "ka")
F32 = jnp.float32
BF16 = jnp.bfloat16
ROWS_BY_ROWS = (((1,), (1,)), ((), ()))


def low_lanes(rows):
    return lax.broadcasted_iota(jnp.int32, (rows, LANES), 1) < HEAD_DIM


def regroup(first, second):
    low = low_lanes(first.shape[0])
    mixed = pltpu.roll(jnp.where(low, second, first), HEAD_DIM, 1)
    return jnp.where(low, first, mixed), jnp.where(low, mixed, second)


def fetch(sources, targets, sems):
    copies = [
        pltpu.make_async_copy(source, target, sems.at[index])
        for index, (source, target) in enumerate(zip(sources, targets))
    ]
    for copy in copies:
        copy.start()
    return copies


def pack_kernel(n_ka, reps, sec, *refs):
    sources, out_ref, (*held, sems) = refs[:6], refs[6], refs[7:]
    for copy in fetch(sources, held, sems):
        copy.wait()
    q_ref, g_ref, k_ref, v_ref, norm_ref, delta_ref = held
    heads, rows = norm_ref.shape
    kept = k_ref.shape[1]
    half = rows // 2
    size = sec + half + 2
    me = lax.axis_index("pb") * n_ka + lax.axis_index("ka")
    slot = lax.rem(me, LANES // half)
    token = lax.broadcasted_iota(jnp.int32, (rows, 2 * LANES), 0)
    lane = lax.broadcasted_iota(jnp.int32, (rows, 2 * LANES), 1)
    quarter = half // 2
    target = (
        lax.div(token, half) * LANES
        + lax.rem(lax.div(token, quarter), 2) * HEAD_DIM
        + slot * quarter
        + lax.rem(token, quarter)
    )
    place = jnp.where(lane == target, 1.0, 0.0).astype(BF16)
    both = jnp.concatenate([norm_ref[...], delta_ref[...]], axis=0)
    moved = jnp.dot(both, place, preferred_element_type=F32)
    stacked = jnp.concatenate(
        [
            moved[:heads, :LANES],
            moved[:heads, LANES:],
            moved[heads:, :LANES],
            moved[heads:, LANES:],
        ],
        axis=0,
    ).astype(BF16)
    row = lax.broadcasted_iota(jnp.int32, (heads * 4, heads * 4), 0)
    col = lax.broadcasted_iota(jnp.int32, (heads * 4, heads * 4), 1)
    inner = lax.rem(row, 4)
    wanted = (lax.rem(inner, 2) * 2 + lax.div(inner, 2)) * heads + lax.div(row, 4)
    pick = jnp.where(col == wanted, 1.0, 0.0).astype(BF16)
    extra = jnp.dot(pick, stacked, preferred_element_type=F32)

    for pair in range(heads // 2):
        cols = slice(pair * LANES, (pair + 1) * LANES)
        queries = regroup(q_ref[:, cols].astype(F32), g_ref[:, cols].astype(F32))
        keys = [
            regroup(k_ref[rep, :, cols].astype(F32), v_ref[rep, :, cols].astype(F32))
            for rep in range(reps)
        ]
        for which in range(2):
            head = 2 * pair + which
            for rep in range(reps):
                base = (head * reps + rep) * size
                side = rep % 2
                key_rows = keys[rep][which]
                if kept < sec:
                    key_rows = jnp.concatenate([key_rows, jnp.zeros((sec - kept, LANES), F32)], axis=0)
                out_ref[base : base + sec, :] = key_rows.astype(BF16)
                out_ref[base + sec : base + sec + half, :] = queries[which][
                    side * half : (side + 1) * half
                ].astype(BF16)
                first = head * 4 + side * 2
                out_ref[base + sec + half : base + size, :] = extra[first : first + 2].astype(BF16)


def split_kernel(count, sec, half, in_ref, own_ref):
    size = sec + half + 2
    quarter = half // 2
    slots = LANES // half
    saved = []
    for group in range(count // slots):
        total = None
        for source in range(group * slots, (group + 1) * slots):
            base = source * size + sec
            for part in range(2):
                row = (part * count + source) * quarter
                own_ref[row : row + quarter, :] = in_ref[
                    base + part * quarter : base + (part + 1) * quarter, :
                ]
            extra = in_ref[base + half : base + half + 2, :].astype(F32)
            total = extra if total is None else total + extra
        saved.append(total)
    pairs = [regroup(saved[group], saved[group + 1]) for group in range(0, len(saved), 2)]
    rows = [pair[part][kind : kind + 1] for kind in range(2) for part in range(2) for pair in pairs]
    base = count * half
    own_ref[base : base + len(rows), :] = jnp.concatenate(rows, axis=0).astype(BF16)


def attend(queries_ref, saved_ref, kv_ref, kt_ref, gq_ref, emit):
    keys = kv_ref.shape[0]
    low = low_lanes(TILE)
    blocks = gq_ref.shape[0]
    rows = TILE // LANES
    saved_ref[...] = queries_ref[blocks * TILE :, :].astype(F32)

    def step(pair):
        sides = []
        for index in (2 * pair, 2 * pair + 1):
            start = index * TILE
            if not isinstance(start, int):
                start = pl.multiple_of(start, TILE)
            block = queries_ref[pl.ds(start, TILE), :].astype(F32)
            queries = jnp.where(low, block * SCALE, 0.0).astype(BF16)
            grads = jnp.where(low, 0.0, block).astype(BF16)
            norm, delta = (
                jnp.concatenate(
                    [
                        saved_ref[pl.ds((kind * blocks + index) * rows + row, 1), :]
                        for row in range(rows)
                    ],
                    axis=1,
                )
                for kind in range(2)
            )
            sides.append((queries, grads, norm * LOG2E, delta))
        totals = [None, None]
        for tile in range(keys // TILE):
            span = slice(tile * TILE, (tile + 1) * TILE)
            kv = kv_ref[span, :]
            part = None
            for side, (queries, grads, norm, delta) in enumerate(sides):
                scores = lax.dot_general(kv, queries, ROWS_BY_ROWS, preferred_element_type=F32)
                grad_probs = lax.dot_general(kv, grads, ROWS_BY_ROWS, preferred_element_type=F32)
                probs = jnp.exp2(scores * LOG2E - norm)
                grad_scores = (probs * (grad_probs - delta)).astype(BF16)
                first = jnp.dot(probs.astype(BF16), grads, preferred_element_type=F32)
                part = first if part is None else part + first
                part += jnp.dot(grad_scores, queries, preferred_element_type=F32)
                more = jnp.dot(kt_ref[:, span], grad_scores, preferred_element_type=F32)
                totals[side] = more if totals[side] is None else totals[side] + more
            emit(span, part)
        for side in range(2):
            gq_ref[2 * pair + side] = totals[side]

    if blocks == 2:
        step(0)
    else:
        lax.fori_loop(0, blocks // 2, lambda pair, _: (step(pair), 0)[1], 0)


def own_kernel(count, sec, half, in_ref, queries_ref, *refs):
    weights, (kv_ref, kt_ref, acc_ref, gqb_ref), near, (gq_ref, saved_ref, sems) = (
        refs[:2],
        refs[2:6],
        refs[6:8],
        refs[8:],
    )
    copies = fetch(weights, near, sems)
    size = sec + half + 2
    per_tile = TILE // sec
    for tile in range(count * sec // TILE):
        span = slice(tile * TILE, (tile + 1) * TILE)
        part = jnp.concatenate(
            [
                in_ref[source * size : source * size + sec, :].astype(F32)
                for source in range(tile * per_tile, (tile + 1) * per_tile)
            ],
            axis=0,
        )
        kv_ref[span, :] = part.astype(BF16)
        kt_ref[:, span] = part.T[:HEAD_DIM].astype(BF16)

    once = gq_ref.shape[0] == 2
    if not once:
        acc_ref[...] = jnp.zeros_like(acc_ref)

    def emit(span, part):
        acc_ref[span, :] = part if once else acc_ref[span, :] + part

    attend(queries_ref, saved_ref, kv_ref, kt_ref, gq_ref, emit)
    gqb_ref[...] = gq_ref[...].astype(BF16)
    for copy in copies:
        copy.wait()


def far_kernel(queries_ref, kv_ref, kt_ref, start_ref, weight_ref, *refs):
    dkv_ref, gq_ref, near_ref, acc_ref, saved_ref, sems = refs
    copies = fetch([weight_ref], [near_ref], sems)
    once = gq_ref.shape[0] == 2
    if not once:
        acc_ref[...] = start_ref[...]

    def emit(span, part):
        if once:
            dkv_ref[span, :] = (start_ref[span, :] + part).astype(BF16)
        else:
            acc_ref[span, :] += part

    attend(queries_ref, saved_ref, kv_ref, kt_ref, gq_ref, emit)
    if not once:
        dkv_ref[...] = acc_ref[...].astype(BF16)
    for copy in copies:
        copy.wait()


def gather_kernel(count, sec, quarter, dkv_ref, gq_ref, other_ref, out_ref):
    size = sec + quarter
    blocks = gq_ref.shape[0]
    for source in range(count):
        out_ref[source * size : source * size + sec, :] = dkv_ref[source * sec : (source + 1) * sec, :]
    for index in range(blocks // 2):
        both = jnp.concatenate(
            [
                gq_ref[block] + other_ref[block].astype(F32)
                for block in (index, index + blocks // 2)
            ],
            axis=0,
        )
        packed = both.T * SCALE
        for offset in range(TILE // quarter):
            base = (index * (TILE // quarter) + offset) * size + sec
            out_ref[base : base + quarter, :] = packed[
                offset * quarter : (offset + 1) * quarter
            ].astype(BF16)


def project_kernel(
    reps, sec, quarter, in_ref, wq_ref, wk_ref, wv_ref, dxq_ref, dxkv_ref, gq_ref, gk_ref, gv_ref
):
    size = sec + quarter
    heads = in_ref.shape[0] // (reps * size)
    for pair in range(heads // 2):
        cols = slice(pair * LANES, (pair + 1) * LANES)
        totals = [[None, None], [None, None]]
        for rep in range(reps):
            bases = [((2 * pair + which) * reps + rep) * size for which in range(2)]
            even, odd = (in_ref[base : base + sec, :].astype(F32) for base in bases)
            grad_key, grad_value = regroup(even, odd)
            span = slice(rep * sec, (rep + 1) * sec)
            gk_ref[span, cols] = grad_key.astype(BF16)
            gv_ref[span, cols] = grad_value.astype(BF16)
            side = 1 - rep % 2
            for which, base in enumerate(bases):
                part = in_ref[base + sec : base + size, :].astype(F32)
                before = totals[side][which]
                totals[side][which] = part if before is None else before + part
        for side in range(2):
            for part, rows in enumerate(regroup(*totals[side])):
                first = (2 * side + part) * quarter
                gq_ref[first : first + quarter, cols] = rows.astype(BF16)

    def times(grads_ref, weight_ref):
        return lax.dot_general(
            grads_ref[...], weight_ref[...], ROWS_BY_ROWS, preferred_element_type=F32
        )

    dxq_ref[...] = times(gq_ref, wq_ref).astype(BF16)
    dxkv_ref[...] = (times(gk_ref, wk_ref) + times(gv_ref, wv_ref)).astype(BF16)


def in_vmem(count):
    return [pl.BlockSpec(memory_space=pltpu.VMEM)] * count


def in_hbm(count):
    return [pl.BlockSpec(memory_space=pltpu.HBM)] * count


def keep_in_hbm(arrays):
    return [pltpu.with_memory_space_constraint(array, pltpu.HBM) for array in arrays]


def exchange(packed, count):
    chunks = packed.reshape(count, packed.shape[0] // (2 * count), 2, LANES)
    return lax.all_to_all(chunks, AXES, 0, 0).reshape(packed.shape)


def local(
    n_ka,
    count,
    query_saved,
    key_saved,
    value_saved,
    out_grad,
    log_norm,
    row_delta,
    weight_query,
    weight_key,
    weight_value,
):
    rows, width = query_saved.shape
    key_rows = key_saved.shape[0]
    heads = width // HEAD_DIM
    reps = count // heads
    kept = key_rows // reps
    sec = -(-kept // 8) * 8
    half = rows // 2
    keys = count * sec
    queries = count * half
    if reps % 2 or queries % (2 * TILE) or keys % TILE:
        raise ValueError("sizes")

    inputs = [
        query_saved,
        out_grad,
        key_saved.reshape(reps, kept, width),
        value_saved.reshape(reps, kept, width),
        log_norm,
        row_delta,
    ]
    sent = pl.pallas_call(
        functools.partial(pack_kernel, n_ka, reps, sec),
        out_shape=pltpu.VMEM((count * (sec + half + 2), LANES), BF16),
        in_specs=in_hbm(6),
        out_specs=in_vmem(1)[0],
        scratch_shapes=[pltpu.VMEM(array.shape, BF16) for array in inputs]
        + [pltpu.SemaphoreType.DMA((6,))],
        compiler_params=PARAMS,
    )(*keep_in_hbm(inputs))
    held = exchange(sent, count)
    own = pl.pallas_call(
        functools.partial(split_kernel, count, sec, half),
        out_shape=pltpu.VMEM((queries + queries * 2 // LANES, LANES), BF16),
        in_specs=in_vmem(1),
        out_specs=in_vmem(1)[0],
        compiler_params=PARAMS,
    )(held)
    twins = [(index, index ^ 1) for index in range(count)]
    far = lax.ppermute(own, AXES, twins)
    work = pl.CostEstimate(
        flops=10 * queries * keys * HEAD_DIM, transcendentals=queries * keys, bytes_accessed=1 << 20
    )
    blocks = queries // TILE
    saved = pltpu.VMEM((2 * queries // LANES, LANES), F32)
    kv, kt, acc, own_part, near_key, near_value = pl.pallas_call(
        functools.partial(own_kernel, count, sec, half),
        out_shape=[
            pltpu.VMEM((keys, LANES), BF16),
            pltpu.VMEM((HEAD_DIM, keys), BF16),
            pltpu.VMEM((keys, LANES), F32),
            pltpu.VMEM((blocks, HEAD_DIM, TILE), BF16),
            pltpu.VMEM(weight_key.shape, BF16),
            pltpu.VMEM(weight_value.shape, BF16),
        ],
        in_specs=in_vmem(2) + in_hbm(2),
        out_specs=in_vmem(6),
        scratch_shapes=[
            pltpu.VMEM((blocks, HEAD_DIM, TILE), F32),
            saved,
            pltpu.SemaphoreType.DMA((2,)),
        ],
        compiler_params=PARAMS,
        cost_estimate=work,
    )(held, own, *keep_in_hbm([weight_key, weight_value]))
    other_part = lax.ppermute(own_part, AXES, twins)
    grad_keyvalue, far_part, near_query = pl.pallas_call(
        far_kernel,
        out_shape=[
            pltpu.VMEM((keys, LANES), BF16),
            pltpu.VMEM((blocks, HEAD_DIM, TILE), F32),
            pltpu.VMEM(weight_query.shape, BF16),
        ],
        in_specs=in_vmem(4) + in_hbm(1),
        out_specs=in_vmem(3),
        scratch_shapes=[pltpu.VMEM((keys, LANES), F32), saved, pltpu.SemaphoreType.DMA((1,))],
        compiler_params=PARAMS,
        cost_estimate=work,
    )(far, kv, kt, acc, *keep_in_hbm([weight_query]))
    grads = pl.pallas_call(
        functools.partial(gather_kernel, count, sec, half // 2),
        out_shape=pltpu.VMEM((count * (sec + half // 2), LANES), BF16),
        in_specs=in_vmem(3),
        out_specs=in_vmem(1)[0],
        compiler_params=PARAMS,
    )(grad_keyvalue, far_part, other_part)
    returned = exchange(grads, count)
    dx_query, dx_keyvalue = pl.pallas_call(
        functools.partial(project_kernel, reps, sec, half // 2),
        out_shape=(
            jax.ShapeDtypeStruct((rows, width), BF16),
            jax.ShapeDtypeStruct((reps * sec, width), BF16),
        ),
        in_specs=in_vmem(4),
        out_specs=tuple(in_vmem(2)),
        scratch_shapes=[
            pltpu.VMEM((rows, width), BF16),
            pltpu.VMEM((reps * sec, width), BF16),
            pltpu.VMEM((reps * sec, width), BF16),
        ],
        compiler_params=PARAMS,
    )(returned, near_query, near_key, near_value)
    if kept != sec:
        dx_keyvalue = dx_keyvalue.reshape(reps, sec, width)[:, :kept].reshape(key_rows, width)
    return dx_query, dx_keyvalue


def solution(mesh):
    n_ka = mesh.shape["ka"]
    count = mesh.shape["pb"] * n_ka
    in_specs = (
        P(("pb", "ka"), None),
        P(("ka", "pb"), None),
        P(("ka", "pb"), None),
        P(("pb", "ka"), None),
        P(None, ("pb", "ka")),
        P(None, ("pb", "ka")),
        P(),
        P(),
        P(),
    )
    out_specs = (P(("pb", "ka"), None), P(("ka", "pb"), None))
    return jax.shard_map(
        functools.partial(local, n_ka, count),
        mesh=mesh,
        in_specs=in_specs,
        out_specs=out_specs,
        check_vma=False,
    )
```

```python
import functools
import math

import jax
import jax.numpy as jnp
from jax import lax
from jax.experimental import pallas as pl
from jax.experimental.pallas import tpu as pltpu
from jax.sharding import PartitionSpec as P

HEAD_DIM = 64
LANES = 2 * HEAD_DIM
SCALE = 1.0 / HEAD_DIM**0.5
LOG2E = math.log2(math.e)
TILE = 256
VMEM_LIMIT = 24 * 1024 * 1024
PARAMS = pltpu.CompilerParams(vmem_limit_bytes=VMEM_LIMIT)
AXES = ("pb", "ka")
F32 = jnp.float32
BF16 = jnp.bfloat16
ROWS_BY_ROWS = (((1,), (1,)), ((), ()))


def low_lanes(rows):
    return lax.broadcasted_iota(jnp.int32, (rows, LANES), 1) < HEAD_DIM


def regroup(first, second):
    low = low_lanes(first.shape[0])
    mixed = pltpu.roll(jnp.where(low, second, first), HEAD_DIM, 1)
    return jnp.where(low, first, mixed), jnp.where(low, mixed, second)


def fetch(sources, targets, sems):
    copies = [
        pltpu.make_async_copy(source, target, sems.at[index])
        for index, (source, target) in enumerate(zip(sources, targets))
    ]
    for copy in copies:
        copy.start()
    return copies


def pack_kernel(n_ka, reps, sec, *refs):
    sources, out_ref, (*held, sems) = refs[:6], refs[6], refs[7:]
    copies = fetch(sources, held, sems)
    norm_ref, delta_ref, q_ref, g_ref, k_ref, v_ref = held

    def arrive(*which):
        for index in which:
            copies[index].wait()

    heads, rows = norm_ref.shape
    kept = k_ref.shape[1]
    half = rows // 2
    quarter = half // 2
    size = sec + half + 2
    me = lax.axis_index("pb") * n_ka + lax.axis_index("ka")
    slot = lax.rem(me, LANES // half)
    token = lax.broadcasted_iota(jnp.int32, (rows, 2 * LANES), 0)
    lane = lax.broadcasted_iota(jnp.int32, (rows, 2 * LANES), 1)
    target = (
        lax.div(token, half) * LANES
        + lax.rem(lax.div(token, quarter), 2) * HEAD_DIM
        + slot * quarter
        + lax.rem(token, quarter)
    )
    place = jnp.where(lane == target, 1.0, 0.0).astype(BF16)
    row = lax.broadcasted_iota(jnp.int32, (heads * 4, heads * 4), 0)
    col = lax.broadcasted_iota(jnp.int32, (heads * 4, heads * 4), 1)
    inner = lax.rem(row, 4)
    wanted = (lax.rem(inner, 2) * 2 + lax.div(inner, 2)) * heads + lax.div(row, 4)
    pick = jnp.where(col == wanted, 1.0, 0.0).astype(BF16)
    arrive(0, 1)
    both = jnp.concatenate([norm_ref[...], delta_ref[...]], axis=0)
    moved = jnp.dot(both, place, preferred_element_type=F32)
    stacked = jnp.concatenate(
        [
            moved[:heads, :LANES],
            moved[:heads, LANES:],
            moved[heads:, :LANES],
            moved[heads:, LANES:],
        ],
        axis=0,
    ).astype(BF16)
    extra = jnp.dot(pick, stacked, preferred_element_type=F32)

    def chunks(pair):
        for which in range(2):
            for rep in range(reps):
                head = 2 * pair + which
                yield which, head, rep, (head * reps + rep) * size

    arrive(2, 3)
    for pair in range(heads // 2):
        cols = slice(pair * LANES, (pair + 1) * LANES)
        queries = regroup(q_ref[:, cols].astype(F32), g_ref[:, cols].astype(F32))
        for which, head, rep, base in chunks(pair):
            side = rep % 2
            out_ref[base + sec : base + sec + half, :] = queries[which][
                side * half : (side + 1) * half
            ].astype(BF16)
            first = head * 4 + side * 2
            out_ref[base + sec + half : base + size, :] = extra[first : first + 2].astype(BF16)
    arrive(4, 5)
    for pair in range(heads // 2):
        cols = slice(pair * LANES, (pair + 1) * LANES)
        keys = [
            regroup(k_ref[rep, :, cols].astype(F32), v_ref[rep, :, cols].astype(F32))
            for rep in range(reps)
        ]
        for which, head, rep, base in chunks(pair):
            key_rows = keys[rep][which]
            if kept < sec:
                key_rows = jnp.concatenate([key_rows, jnp.zeros((sec - kept, LANES), F32)], axis=0)
            out_ref[base : base + sec, :] = key_rows.astype(BF16)


def split_kernel(count, sec, half, in_ref, own_ref):
    size = sec + half + 2
    quarter = half // 2
    slots = LANES // half
    saved = []
    for group in range(count // slots):
        total = None
        for source in range(group * slots, (group + 1) * slots):
            base = source * size + sec
            for part in range(2):
                row = (part * count + source) * quarter
                own_ref[row : row + quarter, :] = in_ref[
                    base + part * quarter : base + (part + 1) * quarter, :
                ]
            extra = in_ref[base + half : base + half + 2, :].astype(F32)
            total = extra if total is None else total + extra
        saved.append(total)
    pairs = [regroup(saved[group], saved[group + 1]) for group in range(0, len(saved), 2)]
    rows = [pair[part][kind : kind + 1] for kind in range(2) for part in range(2) for pair in pairs]
    base = count * half
    own_ref[base : base + len(rows), :] = jnp.concatenate(rows, axis=0).astype(BF16)


def attend(queries_ref, saved_ref, probs_ref, scores_ref, kv_ref, kt_ref, gq_ref, emit):
    keys = kv_ref.shape[0]
    low = low_lanes(TILE)
    blocks = gq_ref.shape[0]
    rows = TILE // LANES
    saved_ref[...] = queries_ref[blocks * TILE :, :].astype(F32)

    def step(pair):
        sides = []
        for index in (2 * pair, 2 * pair + 1):
            start = index * TILE
            if not isinstance(start, int):
                start = pl.multiple_of(start, TILE)
            block = queries_ref[pl.ds(start, TILE), :].astype(F32)
            queries = jnp.where(low, block * SCALE, 0.0).astype(BF16)
            grads = jnp.where(low, 0.0, block).astype(BF16)
            norm, delta = (
                jnp.concatenate(
                    [
                        saved_ref[pl.ds((kind * blocks + index) * rows + row, 1), :]
                        for row in range(rows)
                    ],
                    axis=1,
                )
                for kind in range(2)
            )
            sides.append((queries, grads, norm * LOG2E, delta))
        for tile in range(keys // TILE):
            span = slice(tile * TILE, (tile + 1) * TILE)
            kv = kv_ref[span, :]
            for side, (queries, grads, norm, delta) in enumerate(sides):
                cols = slice(side * TILE, (side + 1) * TILE)
                scores = lax.dot_general(kv, queries, ROWS_BY_ROWS, preferred_element_type=F32)
                grad_probs = lax.dot_general(kv, grads, ROWS_BY_ROWS, preferred_element_type=F32)
                probs = jnp.exp2(scores * LOG2E - norm)
                probs_ref[span, cols] = probs.astype(BF16)
                scores_ref[span, cols] = (probs * (grad_probs - delta)).astype(BF16)
        queries, grads = (jnp.concatenate([side[kind] for side in sides], axis=0) for kind in range(2))
        grad_scores = scores_ref[...]
        grad_query = jnp.dot(kt_ref[...], grad_scores, preferred_element_type=F32)
        for side in range(2):
            gq_ref[2 * pair + side] = grad_query[:, side * TILE : (side + 1) * TILE]
        emit(
            jnp.dot(probs_ref[...], grads, preferred_element_type=F32)
            + jnp.dot(grad_scores, queries, preferred_element_type=F32)
        )

    if blocks == 2:
        step(0)
    else:
        lax.fori_loop(0, blocks // 2, lambda pair, _: (step(pair), 0)[1], 0)


def own_kernel(count, sec, half, in_ref, queries_ref, *refs):
    kv_ref, kt_ref, acc_ref, gqb_ref, gq_ref, *work = refs
    size = sec + half + 2
    per_tile = TILE // sec
    for tile in range(count * sec // TILE):
        span = slice(tile * TILE, (tile + 1) * TILE)
        part = jnp.concatenate(
            [
                in_ref[source * size : source * size + sec, :].astype(F32)
                for source in range(tile * per_tile, (tile + 1) * per_tile)
            ],
            axis=0,
        )
        kv_ref[span, :] = part.astype(BF16)
        kt_ref[:, span] = part.T[:HEAD_DIM].astype(BF16)

    once = gq_ref.shape[0] == 2
    if not once:
        acc_ref[...] = jnp.zeros_like(acc_ref)

    def emit(part):
        acc_ref[...] = part if once else acc_ref[...] + part

    attend(queries_ref, *work, kv_ref, kt_ref, gq_ref, emit)
    gqb_ref[...] = gq_ref[...].astype(BF16)


def far_kernel(queries_ref, kv_ref, kt_ref, start_ref, *refs):
    dkv_ref, gq_ref, acc_ref, *work = refs
    once = gq_ref.shape[0] == 2
    if not once:
        acc_ref[...] = start_ref[...]

    def emit(part):
        if once:
            dkv_ref[...] = (start_ref[...] + part).astype(BF16)
        else:
            acc_ref[...] += part

    attend(queries_ref, *work, kv_ref, kt_ref, gq_ref, emit)
    if not once:
        dkv_ref[...] = acc_ref[...].astype(BF16)


def gather_kernel(count, sec, quarter, dkv_ref, gq_ref, other_ref, out_ref):
    size = sec + quarter
    blocks = gq_ref.shape[0]
    for source in range(count):
        out_ref[source * size : source * size + sec, :] = dkv_ref[source * sec : (source + 1) * sec, :]
    for index in range(blocks // 2):
        both = jnp.concatenate(
            [
                gq_ref[block] + other_ref[block].astype(F32)
                for block in (index, index + blocks // 2)
            ],
            axis=0,
        )
        packed = both.T * SCALE
        for offset in range(TILE // quarter):
            base = (index * (TILE // quarter) + offset) * size + sec
            out_ref[base : base + quarter, :] = packed[
                offset * quarter : (offset + 1) * quarter
            ].astype(BF16)


def project_kernel(reps, sec, quarter, in_ref, wq_ref, wk_ref, wv_ref, dxq_ref, dxkv_ref, *refs):
    gq_ref, gk_ref, gv_ref, qs_ref, kvs_ref, sems = refs
    size = sec + quarter
    heads = in_ref.shape[0] // (reps * size)
    for pair in range(heads // 2):
        cols = slice(pair * LANES, (pair + 1) * LANES)
        totals = [[None, None], [None, None]]
        for rep in range(reps):
            bases = [((2 * pair + which) * reps + rep) * size for which in range(2)]
            even, odd = (in_ref[base : base + sec, :].astype(F32) for base in bases)
            grad_key, grad_value = regroup(even, odd)
            span = slice(rep * sec, (rep + 1) * sec)
            gk_ref[span, cols] = grad_key.astype(BF16)
            gv_ref[span, cols] = grad_value.astype(BF16)
            side = 1 - rep % 2
            for which, base in enumerate(bases):
                part = in_ref[base + sec : base + size, :].astype(F32)
                before = totals[side][which]
                totals[side][which] = part if before is None else before + part
        for side in range(2):
            for part, rows in enumerate(regroup(*totals[side])):
                first = (2 * side + part) * quarter
                gq_ref[first : first + quarter, cols] = rows.astype(BF16)

    def across(grads_ref, weight_ref, span):
        return lax.dot_general(
            grads_ref[...], weight_ref[span, :], ROWS_BY_ROWS, preferred_element_type=F32
        )

    def turned(grads_ref, weight_ref, span):
        return lax.dot_general(
            weight_ref[span, :], grads_ref[...], ROWS_BY_ROWS, preferred_element_type=F32
        ).T

    width = wq_ref.shape[0]
    writes = []

    def write(stage_ref, target_ref, span, value):
        stage_ref[:, span] = value.astype(BF16)
        copy = pltpu.make_async_copy(
            stage_ref.at[:, span], target_ref.at[:, span], sems.at[len(writes)]
        )
        copy.start()
        writes.append(copy)

    step = width // 2
    for first in range(0, width, step):
        span = pl.ds(first, step)
        value = across(gk_ref, wk_ref, span) + turned(gv_ref, wv_ref, span)
        write(kvs_ref, dxkv_ref, span, value)
    write(qs_ref, dxq_ref, pl.ds(0, step), across(gq_ref, wq_ref, pl.ds(0, step)))
    write(qs_ref, dxq_ref, pl.ds(step, step), turned(gq_ref, wq_ref, pl.ds(step, step)))
    for copy in writes:
        copy.wait()


def in_vmem(count):
    return [pl.BlockSpec(memory_space=pltpu.VMEM)] * count


def in_hbm(count):
    return [pl.BlockSpec(memory_space=pltpu.HBM)] * count


def keep_in_hbm(arrays):
    return [pltpu.with_memory_space_constraint(array, pltpu.HBM) for array in arrays]


def exchange(packed, count):
    chunks = packed.reshape(count, packed.shape[0] // (2 * count), 2, LANES)
    return lax.all_to_all(chunks, AXES, 0, 0).reshape(packed.shape)


def local(
    n_ka,
    count,
    query_saved,
    key_saved,
    value_saved,
    out_grad,
    log_norm,
    row_delta,
    weight_query,
    weight_key,
    weight_value,
):
    rows, width = query_saved.shape
    key_rows = key_saved.shape[0]
    heads = width // HEAD_DIM
    reps = count // heads
    kept = key_rows // reps
    sec = -(-kept // 8) * 8
    half = rows // 2
    keys = count * sec
    queries = count * half
    if reps % 2 or queries % (2 * TILE) or keys % TILE:
        raise ValueError("sizes")

    inputs = [
        log_norm,
        row_delta,
        query_saved,
        out_grad,
        key_saved.reshape(reps, kept, width),
        value_saved.reshape(reps, kept, width),
    ]
    sent = pl.pallas_call(
        functools.partial(pack_kernel, n_ka, reps, sec),
        out_shape=pltpu.VMEM((count * (sec + half + 2), LANES), BF16),
        in_specs=in_hbm(6),
        out_specs=in_vmem(1)[0],
        scratch_shapes=[pltpu.VMEM(array.shape, BF16) for array in inputs]
        + [pltpu.SemaphoreType.DMA((6,))],
        compiler_params=PARAMS,
    )(*keep_in_hbm(inputs))
    held = exchange(sent, count)
    own = pl.pallas_call(
        functools.partial(split_kernel, count, sec, half),
        out_shape=pltpu.VMEM((queries + queries * 2 // LANES, LANES), BF16),
        in_specs=in_vmem(1),
        out_specs=in_vmem(1)[0],
        compiler_params=PARAMS,
    )(held)
    twins = [(index, index ^ 1) for index in range(count)]
    far = lax.ppermute(own, AXES, twins)
    work = pl.CostEstimate(
        flops=40 * queries * keys * HEAD_DIM, transcendentals=queries * keys, bytes_accessed=1 << 20
    )
    blocks = queries // TILE
    scratch = [
        pltpu.VMEM((2 * queries // LANES, LANES), F32),
        pltpu.VMEM((keys, 2 * TILE), BF16),
        pltpu.VMEM((keys, 2 * TILE), BF16),
    ]
    kv, kt, acc, own_part = pl.pallas_call(
        functools.partial(own_kernel, count, sec, half),
        out_shape=[
            pltpu.VMEM((keys, LANES), BF16),
            pltpu.VMEM((HEAD_DIM, keys), BF16),
            pltpu.VMEM((keys, LANES), F32),
            pltpu.VMEM((blocks, HEAD_DIM, TILE), BF16),
        ],
        in_specs=in_vmem(2),
        out_specs=in_vmem(4),
        scratch_shapes=[
            pltpu.VMEM((blocks, HEAD_DIM, TILE), F32),
            *scratch,
        ],
        compiler_params=PARAMS,
        cost_estimate=work,
    )(held, own)
    other_part = lax.ppermute(own_part, AXES, twins)
    grad_keyvalue, far_part = pl.pallas_call(
        far_kernel,
        out_shape=[
            pltpu.VMEM((keys, LANES), BF16),
            pltpu.VMEM((blocks, HEAD_DIM, TILE), F32),
        ],
        in_specs=in_vmem(4),
        out_specs=in_vmem(2),
        scratch_shapes=[pltpu.VMEM((keys, LANES), F32), *scratch],
        compiler_params=PARAMS,
        cost_estimate=work,
    )(far, kv, kt, acc)
    grads = pl.pallas_call(
        functools.partial(gather_kernel, count, sec, half // 2),
        out_shape=pltpu.VMEM((count * (sec + half // 2), LANES), BF16),
        in_specs=in_vmem(3),
        out_specs=in_vmem(1)[0],
        compiler_params=PARAMS,
    )(grad_keyvalue, far_part, other_part)
    returned = exchange(grads, count)
    dx_query, dx_keyvalue = pl.pallas_call(
        functools.partial(project_kernel, reps, sec, half // 2),
        out_shape=(
            jax.ShapeDtypeStruct((rows, width), BF16),
            jax.ShapeDtypeStruct((reps * sec, width), BF16),
        ),
        in_specs=in_vmem(4),
        out_specs=tuple(in_hbm(2)),
        scratch_shapes=[
            pltpu.VMEM((rows, width), BF16),
            pltpu.VMEM((reps * sec, width), BF16),
            pltpu.VMEM((reps * sec, width), BF16),
            pltpu.VMEM((rows, width), BF16),
            pltpu.VMEM((reps * sec, width), BF16),
            pltpu.SemaphoreType.DMA((4,)),
        ],
        compiler_params=PARAMS,
    )(
        returned,
        *(
            pltpu.with_memory_space_constraint(weight, pltpu.VMEM)
            for weight in (weight_query, weight_key, weight_value)
        ),
    )
    if kept != sec:
        dx_keyvalue = dx_keyvalue.reshape(reps, sec, width)[:, :kept].reshape(key_rows, width)
    return dx_query, dx_keyvalue


def solution(mesh):
    n_ka = mesh.shape["ka"]
    count = mesh.shape["pb"] * n_ka
    in_specs = (
        P(("pb", "ka"), None),
        P(("ka", "pb"), None),
        P(("ka", "pb"), None),
        P(("pb", "ka"), None),
        P(None, ("pb", "ka")),
        P(None, ("pb", "ka")),
        P(),
        P(),
        P(),
    )
    out_specs = (P(("pb", "ka"), None), P(("ka", "pb"), None))
    return jax.shard_map(
        functools.partial(local, n_ka, count),
        mesh=mesh,
        in_specs=in_specs,
        out_specs=out_specs,
        check_vma=False,
    )
```

```python
import functools
import math

import jax
import jax.numpy as jnp
from jax import lax
from jax.experimental import pallas as pl
from jax.experimental.pallas import tpu as pltpu
from jax.sharding import PartitionSpec as P

HEAD_DIM = 64
LANES = 2 * HEAD_DIM
SCALE = 1.0 / HEAD_DIM**0.5
LOG2E = math.log2(math.e)
TILE = 256
VMEM_LIMIT = 24 * 1024 * 1024
PARAMS = pltpu.CompilerParams(vmem_limit_bytes=VMEM_LIMIT)
AXES = ("pb", "ka")
F32 = jnp.float32
BF16 = jnp.bfloat16
ROWS_BY_ROWS = (((1,), (1,)), ((), ()))


def low_lanes(rows):
    return lax.broadcasted_iota(jnp.int32, (rows, LANES), 1) < HEAD_DIM


def regroup(first, second):
    low = low_lanes(first.shape[0])
    mixed = pltpu.roll(jnp.where(low, second, first), HEAD_DIM, 1)
    return jnp.where(low, first, mixed), jnp.where(low, mixed, second)


def fetch(sources, targets, sems):
    copies = [
        pltpu.make_async_copy(source, target, sems.at[index])
        for index, (source, target) in enumerate(zip(sources, targets))
    ]
    for copy in copies:
        copy.start()
    return copies


def pack_kernel(n_ka, reps, sec, *refs):
    sources, out_ref, (*held, sems) = refs[:6], refs[6], refs[7:]
    copies = fetch(sources, held, sems)
    norm_ref, delta_ref, q_ref, g_ref, k_ref, v_ref = held

    def arrive(*which):
        for index in which:
            copies[index].wait()

    heads, rows = norm_ref.shape
    kept = k_ref.shape[1]
    half = rows // 2
    quarter = half // 2
    size = sec + half + 2
    me = lax.axis_index("pb") * n_ka + lax.axis_index("ka")
    slot = lax.rem(me, LANES // half)
    token = lax.broadcasted_iota(jnp.int32, (rows, 2 * LANES), 0)
    lane = lax.broadcasted_iota(jnp.int32, (rows, 2 * LANES), 1)
    target = (
        lax.div(token, half) * LANES
        + lax.rem(lax.div(token, quarter), 2) * HEAD_DIM
        + slot * quarter
        + lax.rem(token, quarter)
    )
    place = jnp.where(lane == target, 1.0, 0.0).astype(BF16)
    row = lax.broadcasted_iota(jnp.int32, (heads * 4, heads * 4), 0)
    col = lax.broadcasted_iota(jnp.int32, (heads * 4, heads * 4), 1)
    inner = lax.rem(row, 4)
    wanted = (lax.rem(inner, 2) * 2 + lax.div(inner, 2)) * heads + lax.div(row, 4)
    pick = jnp.where(col == wanted, 1.0, 0.0).astype(BF16)
    arrive(0, 1)
    both = jnp.concatenate([norm_ref[...], delta_ref[...]], axis=0)
    moved = jnp.dot(both, place, preferred_element_type=F32)
    stacked = jnp.concatenate(
        [
            moved[:heads, :LANES],
            moved[:heads, LANES:],
            moved[heads:, :LANES],
            moved[heads:, LANES:],
        ],
        axis=0,
    ).astype(BF16)
    extra = jnp.dot(pick, stacked, preferred_element_type=F32)

    def chunks(pair):
        for which in range(2):
            for rep in range(reps):
                head = 2 * pair + which
                yield which, head, rep, (head * reps + rep) * size

    arrive(2, 3)
    for pair in range(heads // 2):
        cols = slice(pair * LANES, (pair + 1) * LANES)
        queries = regroup(q_ref[:, cols].astype(F32), g_ref[:, cols].astype(F32))
        for which, head, rep, base in chunks(pair):
            side = rep % 2
            out_ref[base + sec : base + sec + half, :] = queries[which][
                side * half : (side + 1) * half
            ].astype(BF16)
            first = head * 4 + side * 2
            out_ref[base + sec + half : base + size, :] = extra[first : first + 2].astype(BF16)
    arrive(4, 5)
    for pair in range(heads // 2):
        cols = slice(pair * LANES, (pair + 1) * LANES)
        keys = [
            regroup(k_ref[rep, :, cols].astype(F32), v_ref[rep, :, cols].astype(F32))
            for rep in range(reps)
        ]
        for which, head, rep, base in chunks(pair):
            key_rows = keys[rep][which]
            if kept < sec:
                key_rows = jnp.concatenate([key_rows, jnp.zeros((sec - kept, LANES), F32)], axis=0)
            out_ref[base : base + sec, :] = key_rows.astype(BF16)


def split_kernel(count, sec, half, in_ref, own_ref):
    size = sec + half + 2
    quarter = half // 2
    slots = LANES // half
    saved = []
    for group in range(count // slots):
        total = None
        for source in range(group * slots, (group + 1) * slots):
            base = source * size + sec
            for part in range(2):
                row = (part * count + source) * quarter
                own_ref[row : row + quarter, :] = in_ref[
                    base + part * quarter : base + (part + 1) * quarter, :
                ]
            extra = in_ref[base + half : base + half + 2, :].astype(F32)
            total = extra if total is None else total + extra
        saved.append(total)
    pairs = [regroup(saved[group], saved[group + 1]) for group in range(0, len(saved), 2)]
    rows = [pair[part][kind : kind + 1] for kind in range(2) for part in range(2) for pair in pairs]
    base = count * half
    own_ref[base : base + len(rows), :] = jnp.concatenate(rows, axis=0).astype(BF16)


def attend(queries_ref, saved_ref, probs_ref, scores_ref, kv_ref, kt_ref, gq_ref, emit):
    keys = kv_ref.shape[0]
    low = low_lanes(TILE)
    blocks = gq_ref.shape[0]
    rows = TILE // LANES
    saved_ref[...] = queries_ref[blocks * TILE :, :].astype(F32)

    def step(pair):
        sides = []
        for index in (2 * pair, 2 * pair + 1):
            start = index * TILE
            if not isinstance(start, int):
                start = pl.multiple_of(start, TILE)
            block = queries_ref[pl.ds(start, TILE), :].astype(F32)
            queries = jnp.where(low, block * SCALE, 0.0).astype(BF16)
            grads = jnp.where(low, 0.0, block).astype(BF16)
            norm, delta = (
                jnp.concatenate(
                    [
                        saved_ref[pl.ds((kind * blocks + index) * rows + row, 1), :]
                        for row in range(rows)
                    ],
                    axis=1,
                )
                for kind in range(2)
            )
            sides.append((queries, grads, norm * LOG2E, delta))
        for tile in range(keys // TILE):
            span = slice(tile * TILE, (tile + 1) * TILE)
            kv = kv_ref[span, :]
            for side, (queries, grads, norm, delta) in enumerate(sides):
                cols = slice(side * TILE, (side + 1) * TILE)
                scores = lax.dot_general(kv, queries, ROWS_BY_ROWS, preferred_element_type=F32)
                grad_probs = lax.dot_general(kv, grads, ROWS_BY_ROWS, preferred_element_type=F32)
                probs = jnp.exp2(scores * LOG2E - norm)
                probs_ref[span, cols] = probs.astype(BF16)
                scores_ref[span, cols] = (probs * (grad_probs - delta)).astype(BF16)
        queries, grads = (jnp.concatenate([side[kind] for side in sides], axis=0) for kind in range(2))
        grad_query = None
        for tile in range(keys // TILE):
            span = slice(tile * TILE, (tile + 1) * TILE)
            grad_scores = scores_ref[span, :]
            more = jnp.dot(kt_ref[:, span], grad_scores, preferred_element_type=F32)
            grad_query = more if grad_query is None else grad_query + more
            emit(
                span,
                jnp.dot(probs_ref[span, :], grads, preferred_element_type=F32)
                + jnp.dot(grad_scores, queries, preferred_element_type=F32),
            )
        for side in range(2):
            gq_ref[2 * pair + side] = grad_query[:, side * TILE : (side + 1) * TILE]

    if blocks == 2:
        step(0)
    else:
        lax.fori_loop(0, blocks // 2, lambda pair, _: (step(pair), 0)[1], 0)


def own_kernel(count, sec, half, in_ref, queries_ref, *refs):
    kv_ref, kt_ref, acc_ref, gqb_ref, gq_ref, *work = refs
    size = sec + half + 2
    per_tile = TILE // sec
    for tile in range(count * sec // TILE):
        span = slice(tile * TILE, (tile + 1) * TILE)
        part = jnp.concatenate(
            [
                in_ref[source * size : source * size + sec, :].astype(F32)
                for source in range(tile * per_tile, (tile + 1) * per_tile)
            ],
            axis=0,
        )
        kv_ref[span, :] = part.astype(BF16)
        kt_ref[:, span] = part.T[:HEAD_DIM].astype(BF16)

    once = gq_ref.shape[0] == 2
    if not once:
        acc_ref[...] = jnp.zeros_like(acc_ref)

    def emit(span, part):
        acc_ref[span, :] = part if once else acc_ref[span, :] + part

    attend(queries_ref, *work, kv_ref, kt_ref, gq_ref, emit)
    gqb_ref[...] = gq_ref[...].astype(BF16)


def far_kernel(queries_ref, kv_ref, kt_ref, start_ref, *refs):
    dkv_ref, gq_ref, acc_ref, *work = refs
    once = gq_ref.shape[0] == 2
    if not once:
        acc_ref[...] = start_ref[...]

    def emit(span, part):
        if once:
            dkv_ref[span, :] = (start_ref[span, :] + part).astype(BF16)
        else:
            acc_ref[span, :] += part

    attend(queries_ref, *work, kv_ref, kt_ref, gq_ref, emit)
    if not once:
        dkv_ref[...] = acc_ref[...].astype(BF16)


def gather_kernel(count, sec, quarter, dkv_ref, gq_ref, other_ref, out_ref):
    size = sec + quarter
    blocks = gq_ref.shape[0]
    for source in range(count):
        out_ref[source * size : source * size + sec, :] = dkv_ref[source * sec : (source + 1) * sec, :]
    for index in range(blocks // 2):
        both = jnp.concatenate(
            [
                gq_ref[block] + other_ref[block].astype(F32)
                for block in (index, index + blocks // 2)
            ],
            axis=0,
        )
        packed = both.T * SCALE
        for offset in range(TILE // quarter):
            base = (index * (TILE // quarter) + offset) * size + sec
            out_ref[base : base + quarter, :] = packed[
                offset * quarter : (offset + 1) * quarter
            ].astype(BF16)


def project_kernel(reps, sec, quarter, in_ref, wq_ref, wk_ref, wv_ref, dxq_ref, dxkv_ref, *refs):
    gq_ref, gk_ref, gv_ref, qs_ref, kvs_ref, sems = refs
    size = sec + quarter
    heads = in_ref.shape[0] // (reps * size)
    for pair in range(heads // 2):
        cols = slice(pair * LANES, (pair + 1) * LANES)
        totals = [[None, None], [None, None]]
        for rep in range(reps):
            bases = [((2 * pair + which) * reps + rep) * size for which in range(2)]
            even, odd = (in_ref[base : base + sec, :].astype(F32) for base in bases)
            grad_key, grad_value = regroup(even, odd)
            span = slice(rep * sec, (rep + 1) * sec)
            gk_ref[span, cols] = grad_key.astype(BF16)
            gv_ref[span, cols] = grad_value.astype(BF16)
            side = 1 - rep % 2
            for which, base in enumerate(bases):
                part = in_ref[base + sec : base + size, :].astype(F32)
                before = totals[side][which]
                totals[side][which] = part if before is None else before + part
        for side in range(2):
            for part, rows in enumerate(regroup(*totals[side])):
                first = (2 * side + part) * quarter
                gq_ref[first : first + quarter, cols] = rows.astype(BF16)

    def across(grads_ref, weight_ref, span):
        return lax.dot_general(
            grads_ref[...], weight_ref[span, :], ROWS_BY_ROWS, preferred_element_type=F32
        )

    def turned(grads_ref, weight_ref, span):
        return lax.dot_general(
            weight_ref[span, :], grads_ref[...], ROWS_BY_ROWS, preferred_element_type=F32
        ).T

    width = wq_ref.shape[0]
    writes = []

    def write(stage_ref, target_ref, span, value):
        stage_ref[:, span] = value.astype(BF16)
        copy = pltpu.make_async_copy(
            stage_ref.at[:, span], target_ref.at[:, span], sems.at[len(writes)]
        )
        copy.start()
        writes.append(copy)

    step = width // 2
    depth = 2 * LANES
    for first in range(0, width, step):
        span = pl.ds(first, step)
        left, right = None, None
        for offset in range(0, width, depth):
            cols = pl.ds(offset, depth)
            more = lax.dot_general(gk_ref[:, cols], wk_ref[span, cols], ROWS_BY_ROWS, preferred_element_type=F32)
            left = more if left is None else left + more
            more = lax.dot_general(wv_ref[span, cols], gv_ref[:, cols], ROWS_BY_ROWS, preferred_element_type=F32)
            right = more if right is None else right + more
        write(kvs_ref, dxkv_ref, span, left + right.T)
    left, right = None, None
    for offset in range(0, width, depth):
        cols = pl.ds(offset, depth)
        more = lax.dot_general(gq_ref[:, cols], wq_ref[pl.ds(0, step), cols], ROWS_BY_ROWS, preferred_element_type=F32)
        left = more if left is None else left + more
        more = lax.dot_general(wq_ref[pl.ds(step, step), cols], gq_ref[:, cols], ROWS_BY_ROWS, preferred_element_type=F32)
        right = more if right is None else right + more
    write(qs_ref, dxq_ref, pl.ds(0, step), left)
    write(qs_ref, dxq_ref, pl.ds(step, step), right.T)
    for copy in writes:
        copy.wait()


def in_vmem(count):
    return [pl.BlockSpec(memory_space=pltpu.VMEM)] * count


def in_hbm(count):
    return [pl.BlockSpec(memory_space=pltpu.HBM)] * count


def keep_in_hbm(arrays):
    return [pltpu.with_memory_space_constraint(array, pltpu.HBM) for array in arrays]


def exchange(packed, count):
    chunks = packed.reshape(count, packed.shape[0] // (2 * count), 2, LANES)
    return lax.all_to_all(chunks, AXES, 0, 0).reshape(packed.shape)


def local(
    n_ka,
    count,
    query_saved,
    key_saved,
    value_saved,
    out_grad,
    log_norm,
    row_delta,
    weight_query,
    weight_key,
    weight_value,
):
    rows, width = query_saved.shape
    key_rows = key_saved.shape[0]
    heads = width // HEAD_DIM
    reps = count // heads
    kept = key_rows // reps
    sec = -(-kept // 8) * 8
    half = rows // 2
    keys = count * sec
    queries = count * half
    if reps % 2 or queries % (2 * TILE) or keys % TILE:
        raise ValueError("sizes")

    inputs = [
        log_norm,
        row_delta,
        query_saved,
        out_grad,
        key_saved.reshape(reps, kept, width),
        value_saved.reshape(reps, kept, width),
    ]
    sent = pl.pallas_call(
        functools.partial(pack_kernel, n_ka, reps, sec),
        out_shape=pltpu.VMEM((count * (sec + half + 2), LANES), BF16),
        in_specs=in_hbm(6),
        out_specs=in_vmem(1)[0],
        scratch_shapes=[pltpu.VMEM(array.shape, BF16) for array in inputs]
        + [pltpu.SemaphoreType.DMA((6,))],
        compiler_params=PARAMS,
    )(*keep_in_hbm(inputs))
    held = exchange(sent, count)
    own = pl.pallas_call(
        functools.partial(split_kernel, count, sec, half),
        out_shape=pltpu.VMEM((queries + queries * 2 // LANES, LANES), BF16),
        in_specs=in_vmem(1),
        out_specs=in_vmem(1)[0],
        compiler_params=PARAMS,
    )(held)
    twins = [(index, index ^ 1) for index in range(count)]
    far = lax.ppermute(own, AXES, twins)
    work = pl.CostEstimate(
        flops=40 * queries * keys * HEAD_DIM, transcendentals=queries * keys, bytes_accessed=1 << 20
    )
    blocks = queries // TILE
    scratch = [
        pltpu.VMEM((2 * queries // LANES, LANES), F32),
        pltpu.VMEM((keys, 2 * TILE), BF16),
        pltpu.VMEM((keys, 2 * TILE), BF16),
    ]
    kv, kt, acc, own_part = pl.pallas_call(
        functools.partial(own_kernel, count, sec, half),
        out_shape=[
            pltpu.VMEM((keys, LANES), BF16),
            pltpu.VMEM((HEAD_DIM, keys), BF16),
            pltpu.VMEM((keys, LANES), F32),
            pltpu.VMEM((blocks, HEAD_DIM, TILE), BF16),
        ],
        in_specs=in_vmem(2),
        out_specs=in_vmem(4),
        scratch_shapes=[
            pltpu.VMEM((blocks, HEAD_DIM, TILE), F32),
            *scratch,
        ],
        compiler_params=PARAMS,
        cost_estimate=work,
    )(held, own)
    other_part = lax.ppermute(own_part, AXES, twins)
    grad_keyvalue, far_part = pl.pallas_call(
        far_kernel,
        out_shape=[
            pltpu.VMEM((keys, LANES), BF16),
            pltpu.VMEM((blocks, HEAD_DIM, TILE), F32),
        ],
        in_specs=in_vmem(4),
        out_specs=in_vmem(2),
        scratch_shapes=[pltpu.VMEM((keys, LANES), F32), *scratch],
        compiler_params=PARAMS,
        cost_estimate=work,
    )(far, kv, kt, acc)
    grads = pl.pallas_call(
        functools.partial(gather_kernel, count, sec, half // 2),
        out_shape=pltpu.VMEM((count * (sec + half // 2), LANES), BF16),
        in_specs=in_vmem(3),
        out_specs=in_vmem(1)[0],
        compiler_params=PARAMS,
    )(grad_keyvalue, far_part, other_part)
    returned = exchange(grads, count)
    dx_query, dx_keyvalue = pl.pallas_call(
        functools.partial(project_kernel, reps, sec, half // 2),
        out_shape=(
            jax.ShapeDtypeStruct((rows, width), BF16),
            jax.ShapeDtypeStruct((reps * sec, width), BF16),
        ),
        in_specs=in_vmem(4),
        out_specs=tuple(in_hbm(2)),
        scratch_shapes=[
            pltpu.VMEM((rows, width), BF16),
            pltpu.VMEM((reps * sec, width), BF16),
            pltpu.VMEM((reps * sec, width), BF16),
            pltpu.VMEM((rows, width), BF16),
            pltpu.VMEM((reps * sec, width), BF16),
            pltpu.SemaphoreType.DMA((4,)),
        ],
        compiler_params=PARAMS,
    )(
        returned,
        *(
            pltpu.with_memory_space_constraint(weight, pltpu.VMEM)
            for weight in (weight_query, weight_key, weight_value)
        ),
    )
    if kept != sec:
        dx_keyvalue = dx_keyvalue.reshape(reps, sec, width)[:, :kept].reshape(key_rows, width)
    return dx_query, dx_keyvalue


def solution(mesh):
    n_ka = mesh.shape["ka"]
    count = mesh.shape["pb"] * n_ka
    in_specs = (
        P(("pb", "ka"), None),
        P(("ka", "pb"), None),
        P(("ka", "pb"), None),
        P(("pb", "ka"), None),
        P(None, ("pb", "ka")),
        P(None, ("pb", "ka")),
        P(),
        P(),
        P(),
    )
    out_specs = (P(("pb", "ka"), None), P(("ka", "pb"), None))
    return jax.shard_map(
        functools.partial(local, n_ka, count),
        mesh=mesh,
        in_specs=in_specs,
        out_specs=out_specs,
        check_vma=False,
    )
```

```python
import functools
import math

import jax
import jax.numpy as jnp
from jax import lax
from jax.experimental import pallas as pl
from jax.experimental.pallas import tpu as pltpu
from jax.sharding import Mesh
from jax.sharding import PartitionSpec as P

HEAD_DIM = 64
LANES = 2 * HEAD_DIM
SCALE = 1.0 / HEAD_DIM**0.5
LOG2E = math.log2(math.e)
TILE = 256
VMEM_LIMIT = 24 * 1024 * 1024
PARAMS = pltpu.CompilerParams(vmem_limit_bytes=VMEM_LIMIT)
PARTS = ("pb_hi", "pb_lo", "ka_hi", "ka_lo")
AXES = ("pb_lo", "ka_hi", "ka_lo", "pb_hi")
F32 = jnp.float32
BF16 = jnp.bfloat16
ROWS_BY_ROWS = (((1,), (1,)), ((), ()))


def place_of(head, rep, reps, depth):
    index = head * reps + rep
    rest, twin = index // 2, index % 2
    return (rest // depth * 2 + twin) * depth + rest % depth


def low_lanes(rows):
    return lax.broadcasted_iota(jnp.int32, (rows, LANES), 1) < HEAD_DIM


def regroup(first, second):
    low = low_lanes(first.shape[0])
    mixed = pltpu.roll(jnp.where(low, second, first), HEAD_DIM, 1)
    return jnp.where(low, first, mixed), jnp.where(low, mixed, second)


def fetch(sources, targets, sems):
    copies = [
        pltpu.make_async_copy(source, target, sems.at[index])
        for index, (source, target) in enumerate(zip(sources, targets))
    ]
    for copy in copies:
        copy.start()
    return copies


def pack_kernel(sizes, reps, sec, *refs):
    sources, out_ref, (*held, sems) = refs[:6], refs[6], refs[7:]
    copies = fetch(sources, held, sems)
    norm_ref, delta_ref, q_ref, g_ref, k_ref, v_ref = held

    def arrive(*which):
        for index in which:
            copies[index].wait()

    heads, rows = norm_ref.shape
    kept = k_ref.shape[1]
    half = rows // 2
    quarter = half // 2
    size = sec + half + 2
    depth = sizes["pb_hi"]
    me = 0
    for axis in AXES:
        me = me * sizes[axis] + lax.axis_index(axis)
    slot = lax.rem(me, LANES // half)
    token = lax.broadcasted_iota(jnp.int32, (rows, 2 * LANES), 0)
    lane = lax.broadcasted_iota(jnp.int32, (rows, 2 * LANES), 1)
    target = (
        lax.div(token, half) * LANES
        + lax.rem(lax.div(token, quarter), 2) * HEAD_DIM
        + slot * quarter
        + lax.rem(token, quarter)
    )
    place = jnp.where(lane == target, 1.0, 0.0).astype(BF16)
    row = lax.broadcasted_iota(jnp.int32, (heads * 4, heads * 4), 0)
    col = lax.broadcasted_iota(jnp.int32, (heads * 4, heads * 4), 1)
    inner = lax.rem(row, 4)
    wanted = (lax.rem(inner, 2) * 2 + lax.div(inner, 2)) * heads + lax.div(row, 4)
    pick = jnp.where(col == wanted, 1.0, 0.0).astype(BF16)
    arrive(0, 1)
    both = jnp.concatenate([norm_ref[...], delta_ref[...]], axis=0)
    moved = jnp.dot(both, place, preferred_element_type=F32)
    stacked = jnp.concatenate(
        [
            moved[:heads, :LANES],
            moved[:heads, LANES:],
            moved[heads:, :LANES],
            moved[heads:, LANES:],
        ],
        axis=0,
    ).astype(BF16)
    extra = jnp.dot(pick, stacked, preferred_element_type=F32)

    def chunks(pair):
        for which in range(2):
            for rep in range(reps):
                head = 2 * pair + which
                yield which, head, rep, place_of(head, rep, reps, depth) * size

    arrive(2, 3)
    for pair in range(heads // 2):
        cols = slice(pair * LANES, (pair + 1) * LANES)
        queries = regroup(q_ref[:, cols].astype(F32), g_ref[:, cols].astype(F32))
        for which, head, rep, base in chunks(pair):
            side = rep % 2
            out_ref[base + sec : base + sec + half, :] = queries[which][
                side * half : (side + 1) * half
            ].astype(BF16)
            first = head * 4 + side * 2
            out_ref[base + sec + half : base + size, :] = extra[first : first + 2].astype(BF16)
    arrive(4, 5)
    for pair in range(heads // 2):
        cols = slice(pair * LANES, (pair + 1) * LANES)
        keys = [
            regroup(k_ref[rep, :, cols].astype(F32), v_ref[rep, :, cols].astype(F32))
            for rep in range(reps)
        ]
        for which, head, rep, base in chunks(pair):
            key_rows = keys[rep][which]
            if kept < sec:
                key_rows = jnp.concatenate([key_rows, jnp.zeros((sec - kept, LANES), F32)], axis=0)
            out_ref[base : base + sec, :] = key_rows.astype(BF16)


def split_kernel(count, sec, half, in_ref, own_ref):
    size = sec + half + 2
    quarter = half // 2
    slots = LANES // half
    saved = []
    for group in range(count // slots):
        total = None
        for source in range(group * slots, (group + 1) * slots):
            base = source * size + sec
            for part in range(2):
                row = (part * count + source) * quarter
                own_ref[row : row + quarter, :] = in_ref[
                    base + part * quarter : base + (part + 1) * quarter, :
                ]
            extra = in_ref[base + half : base + half + 2, :].astype(F32)
            total = extra if total is None else total + extra
        saved.append(total)
    pairs = [regroup(saved[group], saved[group + 1]) for group in range(0, len(saved), 2)]
    rows = [pair[part][kind : kind + 1] for kind in range(2) for part in range(2) for pair in pairs]
    base = count * half
    own_ref[base : base + len(rows), :] = jnp.concatenate(rows, axis=0).astype(BF16)


def attend(queries_ref, saved_ref, probs_ref, scores_ref, kv_ref, kt_ref, gq_ref, emit):
    keys = kv_ref.shape[0]
    low = low_lanes(TILE)
    blocks = gq_ref.shape[0]
    rows = TILE // LANES
    saved_ref[...] = queries_ref[blocks * TILE :, :].astype(F32)

    def step(pair):
        sides = []
        for index in (2 * pair, 2 * pair + 1):
            start = index * TILE
            if not isinstance(start, int):
                start = pl.multiple_of(start, TILE)
            block = queries_ref[pl.ds(start, TILE), :].astype(F32)
            queries = jnp.where(low, block * SCALE, 0.0).astype(BF16)
            grads = jnp.where(low, 0.0, block).astype(BF16)
            norm, delta = (
                jnp.concatenate(
                    [
                        saved_ref[pl.ds((kind * blocks + index) * rows + row, 1), :]
                        for row in range(rows)
                    ],
                    axis=1,
                )
                for kind in range(2)
            )
            sides.append((queries, grads, norm * LOG2E, delta))
        for tile in range(keys // TILE):
            span = slice(tile * TILE, (tile + 1) * TILE)
            kv = kv_ref[span, :]
            for side, (queries, grads, norm, delta) in enumerate(sides):
                cols = slice(side * TILE, (side + 1) * TILE)
                scores = lax.dot_general(kv, queries, ROWS_BY_ROWS, preferred_element_type=F32)
                grad_probs = lax.dot_general(kv, grads, ROWS_BY_ROWS, preferred_element_type=F32)
                probs = jnp.exp2(scores * LOG2E - norm)
                probs_ref[span, cols] = probs.astype(BF16)
                scores_ref[span, cols] = (probs * (grad_probs - delta)).astype(BF16)
        queries, grads = (jnp.concatenate([side[kind] for side in sides], axis=0) for kind in range(2))
        grad_query = None
        for tile in range(keys // TILE):
            span = slice(tile * TILE, (tile + 1) * TILE)
            grad_scores = scores_ref[span, :]
            more = jnp.dot(kt_ref[:, span], grad_scores, preferred_element_type=F32)
            grad_query = more if grad_query is None else grad_query + more
            emit(
                span,
                jnp.dot(probs_ref[span, :], grads, preferred_element_type=F32)
                + jnp.dot(grad_scores, queries, preferred_element_type=F32),
            )
        for side in range(2):
            gq_ref[2 * pair + side] = grad_query[:, side * TILE : (side + 1) * TILE]

    if blocks == 2:
        step(0)
    else:
        lax.fori_loop(0, blocks // 2, lambda pair, _: (step(pair), 0)[1], 0)


def own_kernel(count, sec, half, in_ref, queries_ref, *refs):
    kv_ref, kt_ref, acc_ref, gqb_ref, gq_ref, *work = refs
    size = sec + half + 2
    per_tile = TILE // sec
    for tile in range(count * sec // TILE):
        span = slice(tile * TILE, (tile + 1) * TILE)
        part = jnp.concatenate(
            [
                in_ref[source * size : source * size + sec, :].astype(F32)
                for source in range(tile * per_tile, (tile + 1) * per_tile)
            ],
            axis=0,
        )
        kv_ref[span, :] = part.astype(BF16)
        kt_ref[:, span] = part.T[:HEAD_DIM].astype(BF16)

    once = gq_ref.shape[0] == 2
    if not once:
        acc_ref[...] = jnp.zeros_like(acc_ref)

    def emit(span, part):
        acc_ref[span, :] = part if once else acc_ref[span, :] + part

    attend(queries_ref, *work, kv_ref, kt_ref, gq_ref, emit)
    gqb_ref[...] = gq_ref[...].astype(BF16)


def far_kernel(queries_ref, kv_ref, kt_ref, start_ref, *refs):
    dkv_ref, gq_ref, acc_ref, *work = refs
    once = gq_ref.shape[0] == 2
    if not once:
        acc_ref[...] = start_ref[...]

    def emit(span, part):
        if once:
            dkv_ref[span, :] = (start_ref[span, :] + part).astype(BF16)
        else:
            acc_ref[span, :] += part

    attend(queries_ref, *work, kv_ref, kt_ref, gq_ref, emit)
    if not once:
        dkv_ref[...] = acc_ref[...].astype(BF16)


def gather_kernel(count, sec, quarter, dkv_ref, gq_ref, other_ref, out_ref):
    size = sec + quarter
    blocks = gq_ref.shape[0]
    for source in range(count):
        out_ref[source * size : source * size + sec, :] = dkv_ref[source * sec : (source + 1) * sec, :]
    for index in range(blocks // 2):
        both = jnp.concatenate(
            [
                gq_ref[block] + other_ref[block].astype(F32)
                for block in (index, index + blocks // 2)
            ],
            axis=0,
        )
        packed = both.T * SCALE
        for offset in range(TILE // quarter):
            base = (index * (TILE // quarter) + offset) * size + sec
            out_ref[base : base + quarter, :] = packed[
                offset * quarter : (offset + 1) * quarter
            ].astype(BF16)


def project_kernel(depth, reps, sec, quarter, in_ref, wq_ref, wk_ref, wv_ref, dxq_ref, dxkv_ref, *refs):
    gq_ref, gk_ref, gv_ref, qs_ref, kvs_ref, sems = refs
    size = sec + quarter
    heads = in_ref.shape[0] // (reps * size)
    for pair in range(heads // 2):
        cols = slice(pair * LANES, (pair + 1) * LANES)
        totals = [[None, None], [None, None]]
        for rep in range(reps):
            bases = [
                place_of(2 * pair + which, rep, reps, depth) * size for which in range(2)
            ]
            even, odd = (in_ref[base : base + sec, :].astype(F32) for base in bases)
            grad_key, grad_value = regroup(even, odd)
            span = slice(rep * sec, (rep + 1) * sec)
            gk_ref[span, cols] = grad_key.astype(BF16)
            gv_ref[span, cols] = grad_value.astype(BF16)
            side = 1 - rep % 2
            for which, base in enumerate(bases):
                part = in_ref[base + sec : base + size, :].astype(F32)
                before = totals[side][which]
                totals[side][which] = part if before is None else before + part
        for side in range(2):
            for part, rows in enumerate(regroup(*totals[side])):
                first = (2 * side + part) * quarter
                gq_ref[first : first + quarter, cols] = rows.astype(BF16)

    def across(grads_ref, weight_ref, span):
        return lax.dot_general(
            grads_ref[...], weight_ref[span, :], ROWS_BY_ROWS, preferred_element_type=F32
        )

    def turned(grads_ref, weight_ref, span):
        return lax.dot_general(
            weight_ref[span, :], grads_ref[...], ROWS_BY_ROWS, preferred_element_type=F32
        ).T

    width = wq_ref.shape[0]
    writes = []

    def write(stage_ref, target_ref, span, value):
        stage_ref[:, span] = value.astype(BF16)
        copy = pltpu.make_async_copy(
            stage_ref.at[:, span], target_ref.at[:, span], sems.at[len(writes)]
        )
        copy.start()
        writes.append(copy)

    step = width // 2
    depth = 2 * LANES
    for first in range(0, width, step):
        span = pl.ds(first, step)
        left, right = None, None
        for offset in range(0, width, depth):
            cols = pl.ds(offset, depth)
            more = lax.dot_general(gk_ref[:, cols], wk_ref[span, cols], ROWS_BY_ROWS, preferred_element_type=F32)
            left = more if left is None else left + more
            more = lax.dot_general(wv_ref[span, cols], gv_ref[:, cols], ROWS_BY_ROWS, preferred_element_type=F32)
            right = more if right is None else right + more
        write(kvs_ref, dxkv_ref, span, left + right.T)
    left, right = None, None
    for offset in range(0, width, depth):
        cols = pl.ds(offset, depth)
        more = lax.dot_general(gq_ref[:, cols], wq_ref[pl.ds(0, step), cols], ROWS_BY_ROWS, preferred_element_type=F32)
        left = more if left is None else left + more
        more = lax.dot_general(wq_ref[pl.ds(step, step), cols], gq_ref[:, cols], ROWS_BY_ROWS, preferred_element_type=F32)
        right = more if right is None else right + more
    write(qs_ref, dxq_ref, pl.ds(0, step), left)
    write(qs_ref, dxq_ref, pl.ds(step, step), right.T)
    for copy in writes:
        copy.wait()


def in_vmem(count):
    return [pl.BlockSpec(memory_space=pltpu.VMEM)] * count


def in_hbm(count):
    return [pl.BlockSpec(memory_space=pltpu.HBM)] * count


def keep_in_hbm(arrays):
    return [pltpu.with_memory_space_constraint(array, pltpu.HBM) for array in arrays]


def exchange(packed, count):
    chunks = packed.reshape(count, packed.shape[0] // (2 * count), 2, LANES)
    return lax.all_to_all(chunks, AXES, 0, 0).reshape(packed.shape)


def local(
    sizes,
    count,
    query_saved,
    key_saved,
    value_saved,
    out_grad,
    log_norm,
    row_delta,
    weight_query,
    weight_key,
    weight_value,
):
    rows, width = query_saved.shape
    key_rows = key_saved.shape[0]
    heads = width // HEAD_DIM
    reps = count // heads
    kept = key_rows // reps
    sec = -(-kept // 8) * 8
    half = rows // 2
    keys = count * sec
    queries = count * half
    if reps % 2 or queries % (2 * TILE) or keys % TILE:
        raise ValueError("sizes")

    inputs = [
        log_norm,
        row_delta,
        query_saved,
        out_grad,
        key_saved.reshape(reps, kept, width),
        value_saved.reshape(reps, kept, width),
    ]
    sent = pl.pallas_call(
        functools.partial(pack_kernel, sizes, reps, sec),
        out_shape=pltpu.VMEM((count * (sec + half + 2), LANES), BF16),
        in_specs=in_hbm(6),
        out_specs=in_vmem(1)[0],
        scratch_shapes=[pltpu.VMEM(array.shape, BF16) for array in inputs]
        + [pltpu.SemaphoreType.DMA((6,))],
        compiler_params=PARAMS,
    )(*keep_in_hbm(inputs))
    held = exchange(sent, count)
    own = pl.pallas_call(
        functools.partial(split_kernel, count, sec, half),
        out_shape=pltpu.VMEM((queries + queries * 2 // LANES, LANES), BF16),
        in_specs=in_vmem(1),
        out_specs=in_vmem(1)[0],
        compiler_params=PARAMS,
    )(held)
    twins = [(0, 1), (1, 0)]
    far = lax.ppermute(own, "ka_lo", twins)
    work = pl.CostEstimate(
        flops=40 * queries * keys * HEAD_DIM, transcendentals=queries * keys, bytes_accessed=1 << 20
    )
    blocks = queries // TILE
    scratch = [
        pltpu.VMEM((2 * queries // LANES, LANES), F32),
        pltpu.VMEM((keys, 2 * TILE), BF16),
        pltpu.VMEM((keys, 2 * TILE), BF16),
    ]
    kv, kt, acc, own_part = pl.pallas_call(
        functools.partial(own_kernel, count, sec, half),
        out_shape=[
            pltpu.VMEM((keys, LANES), BF16),
            pltpu.VMEM((HEAD_DIM, keys), BF16),
            pltpu.VMEM((keys, LANES), F32),
            pltpu.VMEM((blocks, HEAD_DIM, TILE), BF16),
        ],
        in_specs=in_vmem(2),
        out_specs=in_vmem(4),
        scratch_shapes=[
            pltpu.VMEM((blocks, HEAD_DIM, TILE), F32),
            *scratch,
        ],
        compiler_params=PARAMS,
        cost_estimate=work,
    )(held, own)
    other_part = lax.ppermute(own_part, "ka_lo", twins)
    grad_keyvalue, far_part = pl.pallas_call(
        far_kernel,
        out_shape=[
            pltpu.VMEM((keys, LANES), BF16),
            pltpu.VMEM((blocks, HEAD_DIM, TILE), F32),
        ],
        in_specs=in_vmem(4),
        out_specs=in_vmem(2),
        scratch_shapes=[pltpu.VMEM((keys, LANES), F32), *scratch],
        compiler_params=PARAMS,
        cost_estimate=work,
    )(far, kv, kt, acc)
    grads = pl.pallas_call(
        functools.partial(gather_kernel, count, sec, half // 2),
        out_shape=pltpu.VMEM((count * (sec + half // 2), LANES), BF16),
        in_specs=in_vmem(3),
        out_specs=in_vmem(1)[0],
        compiler_params=PARAMS,
    )(grad_keyvalue, far_part, other_part)
    returned = exchange(grads, count)
    dx_query, dx_keyvalue = pl.pallas_call(
        functools.partial(project_kernel, sizes["pb_hi"], reps, sec, half // 2),
        out_shape=(
            jax.ShapeDtypeStruct((rows, width), BF16),
            jax.ShapeDtypeStruct((reps * sec, width), BF16),
        ),
        in_specs=in_vmem(4),
        out_specs=tuple(in_hbm(2)),
        scratch_shapes=[
            pltpu.VMEM((rows, width), BF16),
            pltpu.VMEM((reps * sec, width), BF16),
            pltpu.VMEM((reps * sec, width), BF16),
            pltpu.VMEM((rows, width), BF16),
            pltpu.VMEM((reps * sec, width), BF16),
            pltpu.SemaphoreType.DMA((4,)),
        ],
        compiler_params=PARAMS,
    )(
        returned,
        *(
            pltpu.with_memory_space_constraint(weight, pltpu.VMEM)
            for weight in (weight_query, weight_key, weight_value)
        ),
    )
    if kept != sec:
        dx_keyvalue = dx_keyvalue.reshape(reps, sec, width)[:, :kept].reshape(key_rows, width)
    return dx_query, dx_keyvalue


def solution(mesh):
    n_pb, n_ka = mesh.shape["pb"], mesh.shape["ka"]
    sizes = dict(zip(PARTS, (n_pb // 2, 2, n_ka // 2, 2)))
    split = Mesh(mesh.devices.reshape(tuple(sizes.values())), PARTS)
    pb, ka = PARTS[:2], PARTS[2:]
    in_specs = (
        P(pb + ka, None),
        P(ka + pb, None),
        P(ka + pb, None),
        P(pb + ka, None),
        P(None, pb + ka),
        P(None, pb + ka),
        P(),
        P(),
        P(),
    )
    out_specs = (P(pb + ka, None), P(ka + pb, None))
    return jax.shard_map(
        functools.partial(local, sizes, n_pb * n_ka),
        mesh=split,
        in_specs=in_specs,
        out_specs=out_specs,
        check_vma=False,
    )
```

```python
import functools
import math

import jax
import jax.numpy as jnp
from jax import lax
from jax.experimental import pallas as pl
from jax.experimental.pallas import tpu as pltpu
from jax.sharding import Mesh
from jax.sharding import PartitionSpec as P

HEAD_DIM = 64
LANES = 2 * HEAD_DIM
SCALE = 1.0 / HEAD_DIM**0.5
LOG2E = math.log2(math.e)
TILE = 256
VMEM_LIMIT = 24 * 1024 * 1024
PARAMS = pltpu.CompilerParams(vmem_limit_bytes=VMEM_LIMIT)
ATTEND_PARAMS = pltpu.CompilerParams(
    vmem_limit_bytes=VMEM_LIMIT
)
PARTS = ("pb_hi", "pb_lo", "ka_hi", "ka_lo")
AXES = ("pb_lo", "ka_hi", "ka_lo", "pb_hi")
F32 = jnp.float32
BF16 = jnp.bfloat16
ROWS_BY_ROWS = (((1,), (1,)), ((), ()))


def place_of(head, rep, reps, depth):
    index = head * reps + rep
    rest, twin = index // 2, index % 2
    return (rest // depth * 2 + twin) * depth + rest % depth


def low_lanes(rows):
    return lax.broadcasted_iota(jnp.int32, (rows, LANES), 1) < HEAD_DIM


def regroup(first, second):
    low = low_lanes(first.shape[0])
    mixed = pltpu.roll(jnp.where(low, second, first), HEAD_DIM, 1)
    return jnp.where(low, first, mixed), jnp.where(low, mixed, second)


def fetch(sources, targets, sems):
    copies = [
        pltpu.make_async_copy(source, target, sems.at[index])
        for index, (source, target) in enumerate(zip(sources, targets))
    ]
    for copy in copies:
        copy.start()
    return copies


def pack_kernel(sizes, reps, sec, *refs):
    sources, out_ref, (*held, sems) = refs[:6], refs[6], refs[7:]
    copies = [
        fetch(
            [source.at[part] for part in range(reps)] if len(source.shape) == 3 else [source],
            [target.at[part] for part in range(reps)] if len(target.shape) == 3 else [target],
            sems.at[index],
        )
        for index, (source, target) in enumerate(zip(sources, held))
    ]
    norm_ref, delta_ref, q_ref, g_ref, k_ref, v_ref = held

    def arrive(*which):
        for index in which:
            for copy in copies[index]:
                copy.wait()

    heads, rows = norm_ref.shape
    kept = k_ref.shape[1]
    half = rows // 2
    quarter = half // 2
    size = sec + half + 2
    depth = sizes["pb_hi"]
    me = 0
    for axis in AXES:
        me = me * sizes[axis] + lax.axis_index(axis)
    slot = lax.rem(me, LANES // half)
    token = lax.broadcasted_iota(jnp.int32, (rows, 2 * LANES), 0)
    lane = lax.broadcasted_iota(jnp.int32, (rows, 2 * LANES), 1)
    target = (
        lax.div(token, half) * LANES
        + lax.rem(lax.div(token, quarter), 2) * HEAD_DIM
        + slot * quarter
        + lax.rem(token, quarter)
    )
    place = jnp.where(lane == target, 1.0, 0.0).astype(BF16)
    row = lax.broadcasted_iota(jnp.int32, (heads * 4, heads * 4), 0)
    col = lax.broadcasted_iota(jnp.int32, (heads * 4, heads * 4), 1)
    inner = lax.rem(row, 4)
    wanted = (lax.rem(inner, 2) * 2 + lax.div(inner, 2)) * heads + lax.div(row, 4)
    pick = jnp.where(col == wanted, 1.0, 0.0).astype(BF16)
    arrive(0, 1)
    both = jnp.concatenate([norm_ref[...], delta_ref[...]], axis=0)
    moved = jnp.dot(both, place, preferred_element_type=F32)
    stacked = jnp.concatenate(
        [
            moved[:heads, :LANES],
            moved[:heads, LANES:],
            moved[heads:, :LANES],
            moved[heads:, LANES:],
        ],
        axis=0,
    ).astype(BF16)
    extra = jnp.dot(pick, stacked, preferred_element_type=F32)

    def chunks(pair):
        for which in range(2):
            for rep in range(reps):
                head = 2 * pair + which
                yield which, head, rep, place_of(head, rep, reps, depth) * size

    arrive(2, 3)
    for pair in range(heads // 2):
        cols = slice(pair * LANES, (pair + 1) * LANES)
        queries = regroup(q_ref[:, cols].astype(F32), g_ref[:, cols].astype(F32))
        for which, head, rep, base in chunks(pair):
            side = rep % 2
            out_ref[base + sec : base + sec + half, :] = queries[which][
                side * half : (side + 1) * half
            ].astype(BF16)
            first = head * 4 + side * 2
            out_ref[base + sec + half : base + size, :] = extra[first : first + 2].astype(BF16)
    arrive(4, 5)
    for pair in range(heads // 2):
        cols = slice(pair * LANES, (pair + 1) * LANES)
        keys = [
            regroup(k_ref[rep, :, cols].astype(F32), v_ref[rep, :, cols].astype(F32))
            for rep in range(reps)
        ]
        for which, head, rep, base in chunks(pair):
            key_rows = keys[rep][which]
            if kept < sec:
                key_rows = jnp.concatenate([key_rows, jnp.zeros((sec - kept, LANES), F32)], axis=0)
            out_ref[base : base + sec, :] = key_rows.astype(BF16)


def split_kernel(count, sec, half, in_ref, own_ref):
    size = sec + half + 2
    quarter = half // 2
    slots = LANES // half
    saved = []
    for group in range(count // slots):
        total = None
        for source in range(group * slots, (group + 1) * slots):
            base = source * size + sec
            for part in range(2):
                row = (part * count + source) * quarter
                own_ref[row : row + quarter, :] = in_ref[
                    base + part * quarter : base + (part + 1) * quarter, :
                ]
            extra = in_ref[base + half : base + half + 2, :].astype(F32)
            total = extra if total is None else total + extra
        saved.append(total)
    pairs = [regroup(saved[group], saved[group + 1]) for group in range(0, len(saved), 2)]
    rows = [pair[part][kind : kind + 1] for kind in range(2) for part in range(2) for pair in pairs]
    base = count * half
    own_ref[base : base + len(rows), :] = jnp.concatenate(rows, axis=0).astype(BF16)


def attend(queries_ref, saved_ref, probs_ref, scores_ref, kv_ref, kt_ref, gq_ref, emit):
    keys = kv_ref.shape[0]
    low = low_lanes(TILE)
    blocks = gq_ref.shape[0]
    rows = TILE // LANES
    saved_ref[...] = queries_ref[blocks * TILE :, :].astype(F32)

    def step(pair):
        sides = []
        for index in (2 * pair, 2 * pair + 1):
            start = index * TILE
            if not isinstance(start, int):
                start = pl.multiple_of(start, TILE)
            block = queries_ref[pl.ds(start, TILE), :].astype(F32)
            queries = jnp.where(low, block * SCALE, 0.0).astype(BF16)
            grads = jnp.where(low, 0.0, block).astype(BF16)
            norm, delta = (
                jnp.concatenate(
                    [
                        saved_ref[pl.ds((kind * blocks + index) * rows + row, 1), :]
                        for row in range(rows)
                    ],
                    axis=1,
                )
                for kind in range(2)
            )
            sides.append((queries, grads, norm * LOG2E, delta))
        for tile in range(keys // TILE):
            span = slice(tile * TILE, (tile + 1) * TILE)
            kv = kv_ref[span, :]
            for side, (queries, grads, norm, delta) in enumerate(sides):
                cols = slice(side * TILE, (side + 1) * TILE)
                scores = lax.dot_general(kv, queries, ROWS_BY_ROWS, preferred_element_type=F32)
                grad_probs = lax.dot_general(kv, grads, ROWS_BY_ROWS, preferred_element_type=F32)
                probs = jnp.exp2(scores * LOG2E - norm)
                probs_ref[span, cols] = probs.astype(BF16)
                scores_ref[span, cols] = (probs * (grad_probs - delta)).astype(BF16)
        queries, grads = (jnp.concatenate([side[kind] for side in sides], axis=0) for kind in range(2))
        grad_query = None
        for tile in range(keys // TILE):
            span = slice(tile * TILE, (tile + 1) * TILE)
            grad_scores = scores_ref[span, :]
            more = jnp.dot(kt_ref[:, span], grad_scores, preferred_element_type=F32)
            grad_query = more if grad_query is None else grad_query + more
            emit(
                span,
                jnp.dot(probs_ref[span, :], grads, preferred_element_type=F32)
                + jnp.dot(grad_scores, queries, preferred_element_type=F32),
            )
        for side in range(2):
            gq_ref[2 * pair + side] = grad_query[:, side * TILE : (side + 1) * TILE]

    if blocks == 2:
        step(0)
    else:
        lax.fori_loop(0, blocks // 2, lambda pair, _: (step(pair), 0)[1], 0)


def own_kernel(count, sec, half, in_ref, queries_ref, *refs):
    kv_ref, kt_ref, acc_ref, gqb_ref, gq_ref, *work = refs
    size = sec + half + 2
    per_tile = TILE // sec
    for tile in range(count * sec // TILE):
        span = slice(tile * TILE, (tile + 1) * TILE)
        part = jnp.concatenate(
            [
                in_ref[source * size : source * size + sec, :].astype(F32)
                for source in range(tile * per_tile, (tile + 1) * per_tile)
            ],
            axis=0,
        )
        kv_ref[span, :] = part.astype(BF16)
        kt_ref[:, span] = part.T[:HEAD_DIM].astype(BF16)

    once = gq_ref.shape[0] == 2
    if not once:
        acc_ref[...] = jnp.zeros_like(acc_ref)

    def emit(span, part):
        acc_ref[span, :] = part if once else acc_ref[span, :] + part

    attend(queries_ref, *work, kv_ref, kt_ref, gq_ref, emit)
    gqb_ref[...] = gq_ref[...].astype(BF16)


def far_kernel(queries_ref, kv_ref, kt_ref, start_ref, *refs):
    dkv_ref, gq_ref, acc_ref, *work = refs
    once = gq_ref.shape[0] == 2
    if not once:
        acc_ref[...] = start_ref[...]

    def emit(span, part):
        if once:
            dkv_ref[span, :] = (start_ref[span, :] + part).astype(BF16)
        else:
            acc_ref[span, :] += part

    attend(queries_ref, *work, kv_ref, kt_ref, gq_ref, emit)
    if not once:
        dkv_ref[...] = acc_ref[...].astype(BF16)


def gather_kernel(count, sec, quarter, dkv_ref, gq_ref, other_ref, out_ref):
    size = sec + quarter
    blocks = gq_ref.shape[0]
    for source in range(count):
        out_ref[source * size : source * size + sec, :] = dkv_ref[source * sec : (source + 1) * sec, :]
    for index in range(blocks // 2):
        both = jnp.concatenate(
            [
                gq_ref[block] + other_ref[block].astype(F32)
                for block in (index, index + blocks // 2)
            ],
            axis=0,
        )
        packed = both.T * SCALE
        for offset in range(TILE // quarter):
            base = (index * (TILE // quarter) + offset) * size + sec
            out_ref[base : base + quarter, :] = packed[
                offset * quarter : (offset + 1) * quarter
            ].astype(BF16)


def project_kernel(depth, reps, sec, quarter, in_ref, wq_ref, wk_ref, wv_ref, dxq_ref, dxkv_ref, *refs):
    gq_ref, gk_ref, gv_ref, qs_ref, kvs_ref, sems = refs
    size = sec + quarter
    heads = in_ref.shape[0] // (reps * size)
    for pair in range(heads // 2):
        cols = slice(pair * LANES, (pair + 1) * LANES)
        totals = [[None, None], [None, None]]
        for rep in range(reps):
            bases = [
                place_of(2 * pair + which, rep, reps, depth) * size for which in range(2)
            ]
            even, odd = (in_ref[base : base + sec, :].astype(F32) for base in bases)
            grad_key, grad_value = regroup(even, odd)
            span = slice(rep * sec, (rep + 1) * sec)
            gk_ref[span, cols] = grad_key.astype(BF16)
            gv_ref[span, cols] = grad_value.astype(BF16)
            side = 1 - rep % 2
            for which, base in enumerate(bases):
                part = in_ref[base + sec : base + size, :].astype(F32)
                before = totals[side][which]
                totals[side][which] = part if before is None else before + part
        for side in range(2):
            for part, rows in enumerate(regroup(*totals[side])):
                first = (2 * side + part) * quarter
                gq_ref[first : first + quarter, cols] = rows.astype(BF16)

    def across(grads_ref, weight_ref, span):
        return lax.dot_general(
            grads_ref[...], weight_ref[span, :], ROWS_BY_ROWS, preferred_element_type=F32
        )

    def turned(grads_ref, weight_ref, span):
        return lax.dot_general(
            weight_ref[span, :], grads_ref[...], ROWS_BY_ROWS, preferred_element_type=F32
        ).T

    width = wq_ref.shape[0]
    writes = []

    def write(stage_ref, target_ref, span, value):
        stage_ref[:, span] = value.astype(BF16)
        copy = pltpu.make_async_copy(
            stage_ref.at[:, span], target_ref.at[:, span], sems.at[len(writes)]
        )
        copy.start()
        writes.append(copy)

    step = width // 2
    depth = 2 * LANES
    for first in range(0, width, step):
        span = pl.ds(first, step)
        left, right = None, None
        for offset in range(0, width, depth):
            cols = pl.ds(offset, depth)
            more = lax.dot_general(gk_ref[:, cols], wk_ref[span, cols], ROWS_BY_ROWS, preferred_element_type=F32)
            left = more if left is None else left + more
            more = lax.dot_general(wv_ref[span, cols], gv_ref[:, cols], ROWS_BY_ROWS, preferred_element_type=F32)
            right = more if right is None else right + more
        write(kvs_ref, dxkv_ref, span, left + right.T)
    left, right = None, None
    for offset in range(0, width, depth):
        cols = pl.ds(offset, depth)
        more = lax.dot_general(gq_ref[:, cols], wq_ref[pl.ds(0, step), cols], ROWS_BY_ROWS, preferred_element_type=F32)
        left = more if left is None else left + more
        more = lax.dot_general(wq_ref[pl.ds(step, step), cols], gq_ref[:, cols], ROWS_BY_ROWS, preferred_element_type=F32)
        right = more if right is None else right + more
    write(qs_ref, dxq_ref, pl.ds(0, step), left)
    write(qs_ref, dxq_ref, pl.ds(step, step), right.T)
    for copy in writes:
        copy.wait()


def in_vmem(count):
    return [pl.BlockSpec(memory_space=pltpu.VMEM)] * count


def in_hbm(count):
    return [pl.BlockSpec(memory_space=pltpu.HBM)] * count


def keep_in_hbm(arrays):
    return [pltpu.with_memory_space_constraint(array, pltpu.HBM) for array in arrays]


def exchange(packed, count):
    chunks = packed.reshape(count, packed.shape[0] // (2 * count), 2, LANES)
    return lax.all_to_all(chunks, AXES, 0, 0).reshape(packed.shape)


def local(
    sizes,
    count,
    query_saved,
    key_saved,
    value_saved,
    out_grad,
    log_norm,
    row_delta,
    weight_query,
    weight_key,
    weight_value,
):
    rows, width = query_saved.shape
    key_rows = key_saved.shape[0]
    heads = width // HEAD_DIM
    reps = count // heads
    kept = key_rows // reps
    sec = -(-kept // 8) * 8
    half = rows // 2
    keys = count * sec
    queries = count * half
    if reps % 2 or queries % (2 * TILE) or keys % TILE:
        raise ValueError("sizes")

    inputs = [
        log_norm,
        row_delta,
        query_saved,
        out_grad,
        key_saved.reshape(reps, kept, width),
        value_saved.reshape(reps, kept, width),
    ]
    sent = pl.pallas_call(
        functools.partial(pack_kernel, sizes, reps, sec),
        out_shape=pltpu.VMEM((count * (sec + half + 2), LANES), BF16),
        in_specs=in_hbm(6),
        out_specs=in_vmem(1)[0],
        scratch_shapes=[pltpu.VMEM(array.shape, BF16) for array in inputs]
        + [pltpu.SemaphoreType.DMA((6, reps))],
        compiler_params=PARAMS,
    )(*keep_in_hbm(inputs))
    held = exchange(sent, count)
    own = pl.pallas_call(
        functools.partial(split_kernel, count, sec, half),
        out_shape=pltpu.VMEM((queries + queries * 2 // LANES, LANES), BF16),
        in_specs=in_vmem(1),
        out_specs=in_vmem(1)[0],
        compiler_params=PARAMS,
    )(held)
    twins = [(0, 1), (1, 0)]
    far = lax.ppermute(own, "ka_lo", twins)
    work = pl.CostEstimate(
        flops=40 * queries * keys * HEAD_DIM, transcendentals=queries * keys, bytes_accessed=1 << 20
    )
    blocks = queries // TILE
    scratch = [
        pltpu.VMEM((2 * queries // LANES, LANES), F32),
        pltpu.VMEM((keys, 2 * TILE), BF16),
        pltpu.VMEM((keys, 2 * TILE), BF16),
    ]
    kv, kt, acc, own_part = pl.pallas_call(
        functools.partial(own_kernel, count, sec, half),
        out_shape=[
            pltpu.VMEM((keys, LANES), BF16),
            pltpu.VMEM((HEAD_DIM, keys), BF16),
            pltpu.VMEM((keys, LANES), F32),
            pltpu.VMEM((blocks, HEAD_DIM, TILE), BF16),
        ],
        in_specs=in_vmem(2),
        out_specs=in_vmem(4),
        scratch_shapes=[
            pltpu.VMEM((blocks, HEAD_DIM, TILE), F32),
            *scratch,
        ],
        compiler_params=ATTEND_PARAMS,
        cost_estimate=work,
    )(held, own)
    other_part = lax.ppermute(own_part, "ka_lo", twins)
    grad_keyvalue, far_part = pl.pallas_call(
        far_kernel,
        out_shape=[
            pltpu.VMEM((keys, LANES), BF16),
            pltpu.VMEM((blocks, HEAD_DIM, TILE), F32),
        ],
        in_specs=in_vmem(4),
        out_specs=in_vmem(2),
        scratch_shapes=[pltpu.VMEM((keys, LANES), F32), *scratch],
        compiler_params=ATTEND_PARAMS,
        cost_estimate=work,
    )(far, kv, kt, acc)
    grads = pl.pallas_call(
        functools.partial(gather_kernel, count, sec, half // 2),
        out_shape=pltpu.VMEM((count * (sec + half // 2), LANES), BF16),
        in_specs=in_vmem(3),
        out_specs=in_vmem(1)[0],
        compiler_params=PARAMS,
    )(grad_keyvalue, far_part, other_part)
    returned = exchange(grads, count)
    dx_query, dx_keyvalue = pl.pallas_call(
        functools.partial(project_kernel, sizes["pb_hi"], reps, sec, half // 2),
        out_shape=(
            jax.ShapeDtypeStruct((rows, width), BF16),
            jax.ShapeDtypeStruct((reps * sec, width), BF16),
        ),
        in_specs=in_vmem(4),
        out_specs=tuple(in_hbm(2)),
        scratch_shapes=[
            pltpu.VMEM((rows, width), BF16),
            pltpu.VMEM((reps * sec, width), BF16),
            pltpu.VMEM((reps * sec, width), BF16),
            pltpu.VMEM((rows, width), BF16),
            pltpu.VMEM((reps * sec, width), BF16),
            pltpu.SemaphoreType.DMA((4,)),
        ],
        compiler_params=PARAMS,
    )(
        returned,
        *(
            pltpu.with_memory_space_constraint(weight, pltpu.VMEM)
            for weight in (weight_query, weight_key, weight_value)
        ),
    )
    if kept != sec:
        dx_keyvalue = dx_keyvalue.reshape(reps, sec, width)[:, :kept].reshape(key_rows, width)
    return dx_query, dx_keyvalue


def solution(mesh):
    n_pb, n_ka = mesh.shape["pb"], mesh.shape["ka"]
    sizes = dict(zip(PARTS, (n_pb // 2, 2, n_ka // 2, 2)))
    split = Mesh(mesh.devices.reshape(tuple(sizes.values())), PARTS)
    pb, ka = PARTS[:2], PARTS[2:]
    in_specs = (
        P(pb + ka, None),
        P(ka + pb, None),
        P(ka + pb, None),
        P(pb + ka, None),
        P(None, pb + ka),
        P(None, pb + ka),
        P(),
        P(),
        P(),
    )
    out_specs = (P(pb + ka, None), P(ka + pb, None))
    return jax.shard_map(
        functools.partial(local, sizes, n_pb * n_ka),
        mesh=split,
        in_specs=in_specs,
        out_specs=out_specs,
        check_vma=False,
    )
```

```python
import functools
import math

import jax
import jax.numpy as jnp
from jax import lax
from jax.experimental import pallas as pl
from jax.experimental.pallas import tpu as pltpu
from jax.sharding import Mesh
from jax.sharding import PartitionSpec as P

HEAD_DIM = 64
LANES = 2 * HEAD_DIM
SCALE = 1.0 / HEAD_DIM**0.5
LOG2E = math.log2(math.e)
TILE = 256
VMEM_LIMIT = 24 * 1024 * 1024
PARAMS = pltpu.CompilerParams(vmem_limit_bytes=VMEM_LIMIT)
ATTEND_PARAMS = pltpu.CompilerParams(
    vmem_limit_bytes=VMEM_LIMIT
)
PARTS = ("pb_hi", "pb_lo", "ka_hi", "ka_lo")
AXES = ("ka_hi", "pb_lo", "ka_lo", "pb_hi")
F32 = jnp.float32
BF16 = jnp.bfloat16
ROWS_BY_ROWS = (((1,), (1,)), ((), ()))


def place_of(head, rep, reps, depth):
    index = head * reps + rep
    rest, twin = index // 2, index % 2
    return (rest // depth * 2 + twin) * depth + rest % depth


def low_lanes(rows):
    return lax.broadcasted_iota(jnp.int32, (rows, LANES), 1) < HEAD_DIM


def regroup(first, second):
    low = low_lanes(first.shape[0])
    mixed = pltpu.roll(jnp.where(low, second, first), HEAD_DIM, 1)
    return jnp.where(low, first, mixed), jnp.where(low, mixed, second)


def fetch(sources, targets, sems):
    copies = [
        pltpu.make_async_copy(source, target, sems.at[index])
        for index, (source, target) in enumerate(zip(sources, targets))
    ]
    for copy in copies:
        copy.start()
    return copies


def pack_kernel(sizes, reps, sec, *refs):
    sources, out_ref, (*held, sems) = refs[:6], refs[6], refs[7:]
    copies = [
        fetch(
            [source.at[part] for part in range(reps)] if len(source.shape) == 3 else [source],
            [target.at[part] for part in range(reps)] if len(target.shape) == 3 else [target],
            sems.at[index],
        )
        for index, (source, target) in enumerate(zip(sources, held))
    ]
    norm_ref, delta_ref, q_ref, g_ref, k_ref, v_ref = held

    def arrive(*which):
        for index in which:
            for copy in copies[index]:
                copy.wait()

    heads, rows = norm_ref.shape
    kept = k_ref.shape[1]
    half = rows // 2
    quarter = half // 2
    size = sec + half + 2
    depth = sizes["pb_hi"]
    me = 0
    for axis in AXES:
        me = me * sizes[axis] + lax.axis_index(axis)
    slot = lax.rem(me, LANES // half)
    token = lax.broadcasted_iota(jnp.int32, (rows, 2 * LANES), 0)
    lane = lax.broadcasted_iota(jnp.int32, (rows, 2 * LANES), 1)
    target = (
        lax.div(token, half) * LANES
        + lax.rem(lax.div(token, quarter), 2) * HEAD_DIM
        + slot * quarter
        + lax.rem(token, quarter)
    )
    place = jnp.where(lane == target, 1.0, 0.0).astype(BF16)
    row = lax.broadcasted_iota(jnp.int32, (heads * 4, heads * 4), 0)
    col = lax.broadcasted_iota(jnp.int32, (heads * 4, heads * 4), 1)
    inner = lax.rem(row, 4)
    wanted = (lax.rem(inner, 2) * 2 + lax.div(inner, 2)) * heads + lax.div(row, 4)
    pick = jnp.where(col == wanted, 1.0, 0.0).astype(BF16)
    arrive(0, 1)
    both = jnp.concatenate([norm_ref[...], delta_ref[...]], axis=0)
    moved = jnp.dot(both, place, preferred_element_type=F32)
    stacked = jnp.concatenate(
        [
            moved[:heads, :LANES],
            moved[:heads, LANES:],
            moved[heads:, :LANES],
            moved[heads:, LANES:],
        ],
        axis=0,
    ).astype(BF16)
    extra = jnp.dot(pick, stacked, preferred_element_type=F32)

    def chunks(pair):
        for which in range(2):
            for rep in range(reps):
                head = 2 * pair + which
                yield which, head, rep, place_of(head, rep, reps, depth) * size

    arrive(2, 3)
    for pair in range(heads // 2):
        cols = slice(pair * LANES, (pair + 1) * LANES)
        queries = regroup(q_ref[:, cols].astype(F32), g_ref[:, cols].astype(F32))
        for which, head, rep, base in chunks(pair):
            side = rep % 2
            out_ref[base + sec : base + sec + half, :] = queries[which][
                side * half : (side + 1) * half
            ].astype(BF16)
            first = head * 4 + side * 2
            out_ref[base + sec + half : base + size, :] = extra[first : first + 2].astype(BF16)
    arrive(4, 5)
    for pair in range(heads // 2):
        cols = slice(pair * LANES, (pair + 1) * LANES)
        keys = [
            regroup(k_ref[rep, :, cols].astype(F32), v_ref[rep, :, cols].astype(F32))
            for rep in range(reps)
        ]
        for which, head, rep, base in chunks(pair):
            key_rows = keys[rep][which]
            if kept < sec:
                key_rows = jnp.concatenate([key_rows, jnp.zeros((sec - kept, LANES), F32)], axis=0)
            out_ref[base : base + sec, :] = key_rows.astype(BF16)


def split_kernel(count, sec, half, in_ref, own_ref):
    size = sec + half + 2
    quarter = half // 2
    slots = LANES // half
    saved = []
    for group in range(count // slots):
        total = None
        for source in range(group * slots, (group + 1) * slots):
            base = source * size + sec
            for part in range(2):
                row = (part * count + source) * quarter
                own_ref[row : row + quarter, :] = in_ref[
                    base + part * quarter : base + (part + 1) * quarter, :
                ]
            extra = in_ref[base + half : base + half + 2, :].astype(F32)
            total = extra if total is None else total + extra
        saved.append(total)
    pairs = [regroup(saved[group], saved[group + 1]) for group in range(0, len(saved), 2)]
    rows = [pair[part][kind : kind + 1] for kind in range(2) for part in range(2) for pair in pairs]
    base = count * half
    own_ref[base : base + len(rows), :] = jnp.concatenate(rows, axis=0).astype(BF16)


def attend(queries_ref, saved_ref, probs_ref, scores_ref, kv_ref, kt_ref, gq_ref, emit):
    keys = kv_ref.shape[0]
    low = low_lanes(TILE)
    blocks = gq_ref.shape[0]
    rows = TILE // LANES
    saved_ref[...] = queries_ref[blocks * TILE :, :].astype(F32)

    def step(pair):
        sides = []
        for index in (2 * pair, 2 * pair + 1):
            start = index * TILE
            if not isinstance(start, int):
                start = pl.multiple_of(start, TILE)
            block = queries_ref[pl.ds(start, TILE), :].astype(F32)
            queries = jnp.where(low, block * SCALE, 0.0).astype(BF16)
            grads = jnp.where(low, 0.0, block).astype(BF16)
            norm, delta = (
                jnp.concatenate(
                    [
                        saved_ref[pl.ds((kind * blocks + index) * rows + row, 1), :]
                        for row in range(rows)
                    ],
                    axis=1,
                )
                for kind in range(2)
            )
            sides.append((queries, grads, norm * LOG2E, delta))
        for tile in range(keys // TILE):
            span = slice(tile * TILE, (tile + 1) * TILE)
            kv = kv_ref[span, :]
            for side, (queries, grads, norm, delta) in enumerate(sides):
                cols = slice(side * TILE, (side + 1) * TILE)
                scores = lax.dot_general(kv, queries, ROWS_BY_ROWS, preferred_element_type=F32)
                grad_probs = lax.dot_general(kv, grads, ROWS_BY_ROWS, preferred_element_type=F32)
                probs = jnp.exp2(scores * LOG2E - norm)
                probs_ref[span, cols] = probs.astype(BF16)
                scores_ref[span, cols] = (probs * (grad_probs - delta)).astype(BF16)
        queries, grads = (jnp.concatenate([side[kind] for side in sides], axis=0) for kind in range(2))
        grad_query = None
        for tile in range(keys // TILE):
            span = slice(tile * TILE, (tile + 1) * TILE)
            grad_scores = scores_ref[span, :]
            more = jnp.dot(kt_ref[:, span], grad_scores, preferred_element_type=F32)
            grad_query = more if grad_query is None else grad_query + more
            emit(
                span,
                jnp.dot(probs_ref[span, :], grads, preferred_element_type=F32)
                + jnp.dot(grad_scores, queries, preferred_element_type=F32),
            )
        for side in range(2):
            gq_ref[2 * pair + side] = grad_query[:, side * TILE : (side + 1) * TILE]

    if blocks == 2:
        step(0)
    else:
        lax.fori_loop(0, blocks // 2, lambda pair, _: (step(pair), 0)[1], 0)


def own_kernel(count, sec, half, in_ref, queries_ref, *refs):
    kv_ref, kt_ref, acc_ref, gqb_ref, gq_ref, *work = refs
    size = sec + half + 2
    per_tile = TILE // sec
    for tile in range(count * sec // TILE):
        span = slice(tile * TILE, (tile + 1) * TILE)
        part = jnp.concatenate(
            [
                in_ref[source * size : source * size + sec, :].astype(F32)
                for source in range(tile * per_tile, (tile + 1) * per_tile)
            ],
            axis=0,
        )
        kv_ref[span, :] = part.astype(BF16)
        kt_ref[:, span] = part.T[:HEAD_DIM].astype(BF16)

    once = gq_ref.shape[0] == 2
    if not once:
        acc_ref[...] = jnp.zeros_like(acc_ref)

    def emit(span, part):
        acc_ref[span, :] = part if once else acc_ref[span, :] + part

    attend(queries_ref, *work, kv_ref, kt_ref, gq_ref, emit)
    gqb_ref[...] = gq_ref[...].astype(BF16)


def far_kernel(queries_ref, kv_ref, kt_ref, start_ref, *refs):
    dkv_ref, gq_ref, acc_ref, *work = refs
    once = gq_ref.shape[0] == 2
    if not once:
        acc_ref[...] = start_ref[...]

    def emit(span, part):
        if once:
            dkv_ref[span, :] = (start_ref[span, :] + part).astype(BF16)
        else:
            acc_ref[span, :] += part

    attend(queries_ref, *work, kv_ref, kt_ref, gq_ref, emit)
    if not once:
        dkv_ref[...] = acc_ref[...].astype(BF16)


def gather_kernel(count, sec, quarter, dkv_ref, gq_ref, other_ref, out_ref):
    size = sec + quarter
    blocks = gq_ref.shape[0]
    for source in range(count):
        out_ref[source * size : source * size + sec, :] = dkv_ref[source * sec : (source + 1) * sec, :]
    for index in range(blocks // 2):
        both = jnp.concatenate(
            [
                gq_ref[block] + other_ref[block].astype(F32)
                for block in (index, index + blocks // 2)
            ],
            axis=0,
        )
        packed = both.T * SCALE
        for offset in range(TILE // quarter):
            base = (index * (TILE // quarter) + offset) * size + sec
            out_ref[base : base + quarter, :] = packed[
                offset * quarter : (offset + 1) * quarter
            ].astype(BF16)


def project_kernel(depth, reps, sec, quarter, in_ref, wq_ref, wk_ref, wv_ref, dxq_ref, dxkv_ref, *refs):
    gq_ref, gk_ref, gv_ref, qs_ref, kvs_ref, sems = refs
    size = sec + quarter
    heads = in_ref.shape[0] // (reps * size)
    for pair in range(heads // 2):
        cols = slice(pair * LANES, (pair + 1) * LANES)
        totals = [[None, None], [None, None]]
        for rep in range(reps):
            bases = [
                place_of(2 * pair + which, rep, reps, depth) * size for which in range(2)
            ]
            even, odd = (in_ref[base : base + sec, :].astype(F32) for base in bases)
            grad_key, grad_value = regroup(even, odd)
            span = slice(rep * sec, (rep + 1) * sec)
            gk_ref[span, cols] = grad_key.astype(BF16)
            gv_ref[span, cols] = grad_value.astype(BF16)
            side = 1 - rep % 2
            for which, base in enumerate(bases):
                part = in_ref[base + sec : base + size, :].astype(F32)
                before = totals[side][which]
                totals[side][which] = part if before is None else before + part
        for side in range(2):
            for part, rows in enumerate(regroup(*totals[side])):
                first = (2 * side + part) * quarter
                gq_ref[first : first + quarter, cols] = rows.astype(BF16)

    def across(grads_ref, weight_ref, span):
        return lax.dot_general(
            grads_ref[...], weight_ref[span, :], ROWS_BY_ROWS, preferred_element_type=F32
        )

    def turned(grads_ref, weight_ref, span):
        return lax.dot_general(
            weight_ref[span, :], grads_ref[...], ROWS_BY_ROWS, preferred_element_type=F32
        ).T

    width = wq_ref.shape[0]
    writes = []

    def write(stage_ref, target_ref, span, value):
        stage_ref[:, span] = value.astype(BF16)
        copy = pltpu.make_async_copy(
            stage_ref.at[:, span], target_ref.at[:, span], sems.at[len(writes)]
        )
        copy.start()
        writes.append(copy)

    step = width // 2
    depth = 2 * LANES
    for first in range(0, width, step):
        span = pl.ds(first, step)
        left, right = None, None
        for offset in range(0, width, depth):
            cols = pl.ds(offset, depth)
            more = lax.dot_general(gk_ref[:, cols], wk_ref[span, cols], ROWS_BY_ROWS, preferred_element_type=F32)
            left = more if left is None else left + more
            more = lax.dot_general(wv_ref[span, cols], gv_ref[:, cols], ROWS_BY_ROWS, preferred_element_type=F32)
            right = more if right is None else right + more
        write(kvs_ref, dxkv_ref, span, left + right.T)
    left, right = None, None
    for offset in range(0, width, depth):
        cols = pl.ds(offset, depth)
        more = lax.dot_general(gq_ref[:, cols], wq_ref[pl.ds(0, step), cols], ROWS_BY_ROWS, preferred_element_type=F32)
        left = more if left is None else left + more
        more = lax.dot_general(wq_ref[pl.ds(step, step), cols], gq_ref[:, cols], ROWS_BY_ROWS, preferred_element_type=F32)
        right = more if right is None else right + more
    write(qs_ref, dxq_ref, pl.ds(0, step), left)
    write(qs_ref, dxq_ref, pl.ds(step, step), right.T)
    for copy in writes:
        copy.wait()


def in_vmem(count):
    return [pl.BlockSpec(memory_space=pltpu.VMEM)] * count


def in_hbm(count):
    return [pl.BlockSpec(memory_space=pltpu.HBM)] * count


def keep_in_hbm(arrays):
    return [pltpu.with_memory_space_constraint(array, pltpu.HBM) for array in arrays]


def exchange(packed, count):
    chunks = packed.reshape(count, packed.shape[0] // (2 * count), 2, LANES)
    return lax.all_to_all(chunks, AXES, 0, 0).reshape(packed.shape)


def local(
    sizes,
    count,
    query_saved,
    key_saved,
    value_saved,
    out_grad,
    log_norm,
    row_delta,
    weight_query,
    weight_key,
    weight_value,
):
    rows, width = query_saved.shape
    key_rows = key_saved.shape[0]
    heads = width // HEAD_DIM
    reps = count // heads
    kept = key_rows // reps
    sec = -(-kept // 8) * 8
    half = rows // 2
    keys = count * sec
    queries = count * half
    if reps % 2 or queries % (2 * TILE) or keys % TILE:
        raise ValueError("sizes")

    inputs = [
        log_norm,
        row_delta,
        query_saved,
        out_grad,
        key_saved.reshape(reps, kept, width),
        value_saved.reshape(reps, kept, width),
    ]
    sent = pl.pallas_call(
        functools.partial(pack_kernel, sizes, reps, sec),
        out_shape=pltpu.VMEM((count * (sec + half + 2), LANES), BF16),
        in_specs=in_hbm(6),
        out_specs=in_vmem(1)[0],
        scratch_shapes=[pltpu.VMEM(array.shape, BF16) for array in inputs]
        + [pltpu.SemaphoreType.DMA((6, reps))],
        compiler_params=PARAMS,
    )(*keep_in_hbm(inputs))
    held = exchange(sent, count)
    own = pl.pallas_call(
        functools.partial(split_kernel, count, sec, half),
        out_shape=pltpu.VMEM((queries + queries * 2 // LANES, LANES), BF16),
        in_specs=in_vmem(1),
        out_specs=in_vmem(1)[0],
        compiler_params=PARAMS,
    )(held)
    twins = [(0, 1), (1, 0)]
    far = lax.ppermute(own, "ka_lo", twins)
    work = pl.CostEstimate(
        flops=40 * queries * keys * HEAD_DIM, transcendentals=queries * keys, bytes_accessed=1 << 20
    )
    blocks = queries // TILE
    scratch = [
        pltpu.VMEM((2 * queries // LANES, LANES), F32),
        pltpu.VMEM((keys, 2 * TILE), BF16),
        pltpu.VMEM((keys, 2 * TILE), BF16),
    ]
    kv, kt, acc, own_part = pl.pallas_call(
        functools.partial(own_kernel, count, sec, half),
        out_shape=[
            pltpu.VMEM((keys, LANES), BF16),
            pltpu.VMEM((HEAD_DIM, keys), BF16),
            pltpu.VMEM((keys, LANES), F32),
            pltpu.VMEM((blocks, HEAD_DIM, TILE), BF16),
        ],
        in_specs=in_vmem(2),
        out_specs=in_vmem(4),
        scratch_shapes=[
            pltpu.VMEM((blocks, HEAD_DIM, TILE), F32),
            *scratch,
        ],
        compiler_params=ATTEND_PARAMS,
        cost_estimate=work,
    )(held, own)
    other_part = lax.ppermute(own_part, "ka_lo", twins)
    grad_keyvalue, far_part = pl.pallas_call(
        far_kernel,
        out_shape=[
            pltpu.VMEM((keys, LANES), BF16),
            pltpu.VMEM((blocks, HEAD_DIM, TILE), F32),
        ],
        in_specs=in_vmem(4),
        out_specs=in_vmem(2),
        scratch_shapes=[pltpu.VMEM((keys, LANES), F32), *scratch],
        compiler_params=ATTEND_PARAMS,
        cost_estimate=work,
    )(far, kv, kt, acc)
    grads = pl.pallas_call(
        functools.partial(gather_kernel, count, sec, half // 2),
        out_shape=pltpu.VMEM((count * (sec + half // 2), LANES), BF16),
        in_specs=in_vmem(3),
        out_specs=in_vmem(1)[0],
        compiler_params=PARAMS,
    )(grad_keyvalue, far_part, other_part)
    returned = exchange(grads, count)
    dx_query, dx_keyvalue = pl.pallas_call(
        functools.partial(project_kernel, sizes["pb_hi"], reps, sec, half // 2),
        out_shape=(
            jax.ShapeDtypeStruct((rows, width), BF16),
            jax.ShapeDtypeStruct((reps * sec, width), BF16),
        ),
        in_specs=in_vmem(4),
        out_specs=tuple(in_hbm(2)),
        scratch_shapes=[
            pltpu.VMEM((rows, width), BF16),
            pltpu.VMEM((reps * sec, width), BF16),
            pltpu.VMEM((reps * sec, width), BF16),
            pltpu.VMEM((rows, width), BF16),
            pltpu.VMEM((reps * sec, width), BF16),
            pltpu.SemaphoreType.DMA((4,)),
        ],
        compiler_params=PARAMS,
    )(
        returned,
        *(
            pltpu.with_memory_space_constraint(weight, pltpu.VMEM)
            for weight in (weight_query, weight_key, weight_value)
        ),
    )
    if kept != sec:
        dx_keyvalue = dx_keyvalue.reshape(reps, sec, width)[:, :kept].reshape(key_rows, width)
    return dx_query, dx_keyvalue


def solution(mesh):
    n_pb, n_ka = mesh.shape["pb"], mesh.shape["ka"]
    sizes = dict(zip(PARTS, (n_pb // 2, 2, n_ka // 2, 2)))
    split = Mesh(mesh.devices.reshape(tuple(sizes.values())), PARTS)
    pb, ka = PARTS[:2], PARTS[2:]
    in_specs = (
        P(pb + ka, None),
        P(ka + pb, None),
        P(ka + pb, None),
        P(pb + ka, None),
        P(None, pb + ka),
        P(None, pb + ka),
        P(),
        P(),
        P(),
    )
    out_specs = (P(pb + ka, None), P(ka + pb, None))
    return jax.shard_map(
        functools.partial(local, sizes, n_pb * n_ka),
        mesh=split,
        in_specs=in_specs,
        out_specs=out_specs,
        check_vma=False,
    )
```
